32 devices in a mesh: grp: 4 (over y, x), gx: 2 (over core), gy: 4 (over z).
Axes of the slice: x: 2, y: 2, z: 4, core: 2. Of those that a mesh axis runs over, the one named last changes fastest.
Arguments:
- velocity: float32 [3, 32, 32, 128], P(None, ('grp', 'gx'), 'gy'), may hold values from -12 to 12
- first_weight: bfloat16 [3, 3, 3, 64, 9], replicated, may hold values from -0.375 to 0.375
- first_bias: float32 [64], replicated, may hold values from -3 to 3
- second_weight: bfloat16 [3, 3, 3, 64, 64], replicated, may hold values from -0.15625 to 0.15625
- second_bias: float32 [64], replicated, may hold values from -3 to 3
- third_weight: bfloat16 [3, 3, 3, 64, 64], replicated, may hold values from -0.15625 to 0.15625
- third_bias: float32 [64], replicated, may hold values from -3 to 3
- last_weight: bfloat16 [3, 3, 3, 6, 64], replicated, may hold values from -0.15625 to 0.15625
Outputs:
- updated: float32 [3, 32, 32, 128], P(None, ('grp', 'gx'), 'gy')
- stress: float32 [6, 32, 32, 128], P(None, ('grp', 'gx'), 'gy')
The draws below stay inside these ranges and needn't reach their ends.
All inputs are finite; a program needn't handle non-finite values.
Results may differ from the reference program's by a relative error of at most 0.002.
The reference program's roundings to bfloat16 on the way (of `features`, `layer_one`, `layer_two` and `layer_three`) count: a program that leaves them out, or rounds other values in their place, can miss the bound.
Values may be sent and summed in bfloat16 or wider, within the bound.
No kernel may reach another device: no remote copies, remote signals or barrier semaphores. Data moves between devices by JAX's collectives and lax.ppermute only.
A program may use at most 192 MiB of HBM per device.

```python
import jax
import jax.numpy as jnp
from jax import lax

CHANNELS = 64
CX = 4
NZ = 128
NX = 32
NY = 32


def draw_velocity(key, part):
    first_key = jax.random.fold_in(key, 11)
    second_key = jax.random.fold_in(key, 12)
    noise = jax.random.truncated_normal(first_key, -4.0, 4.0, (3, NX, NY, NZ), jnp.float32)
    position = jnp.arange(NX, dtype=jnp.float32) / NX
    columns = jax.random.uniform(second_key, (NY,), jnp.float32)
    amplitude = 0.5 * (10.0 ** (0.5 * position))[:, None] * (10.0 ** (0.25 * columns))[None, :]
    return (noise * amplitude[None, :, :, None]).astype(jnp.float32)


def bell_draw(key, dims, width, bound, held_as=jnp.bfloat16):
    return jnp.clip(width * jax.random.normal(key, dims, jnp.float32), -bound, bound).astype(held_as)


def setup_inputs(seed: int = 0) -> dict:
    seeds = jax.random.split(jax.random.key(seed), 9)
    return {
        "velocity": draw_velocity(jax.random.fold_in(seeds[8], 71), 0),
        "first_weight": bell_draw(seeds[1], (3, 3, 3, CHANNELS, 9), (27 * 9) ** -0.5, 0.375),
        "first_bias": bell_draw(seeds[2], (CHANNELS,), 0.5, 3.0, jnp.float32),
        "second_weight": bell_draw(seeds[3], (3, 3, 3, CHANNELS, CHANNELS), (27 * CHANNELS) ** -0.5, 0.15625),
        "second_bias": bell_draw(seeds[4], (CHANNELS,), 0.5, 3.0, jnp.float32),
        "third_weight": bell_draw(seeds[5], (3, 3, 3, CHANNELS, CHANNELS), (27 * CHANNELS) ** -0.5, 0.15625),
        "third_bias": bell_draw(seeds[6], (CHANNELS,), 0.5, 3.0, jnp.float32),
        "last_weight": bell_draw(seeds[7], (3, 3, 3, 6, CHANNELS), (27 * CHANNELS) ** -0.5, 0.15625),
    }


time_step = 0.1
viscosity = 0.05
power_input = 5.0
pairing = ((0, 3, 4), (3, 1, 5), (4, 5, 2))


def convolve(padded, weight, offset):
    in_width, extent_x, extent_y, depth_z = padded.shape
    out_width = weight.shape[3]
    inner_x = extent_x - 2
    inner_y = extent_y - 2
    stacked = jnp.concatenate([jnp.roll(padded, 1, axis=3), padded, jnp.roll(padded, -1, axis=3)], axis=0)
    summed = jnp.zeros((out_width, inner_x * inner_y * depth_z), jnp.float32)
    for shift_x in range(3):
        for shift_y in range(3):
            window = stacked[:, shift_x:shift_x + inner_x, shift_y:shift_y + inner_y, :].reshape(3 * in_width, inner_x * inner_y * depth_z)
            kernel = jnp.transpose(weight[shift_x, shift_y], (1, 0, 2)).reshape(out_width, 3 * in_width)
            summed = summed + jnp.dot(kernel, window, preferred_element_type=jnp.float32)
    summed = summed + offset[:, None]
    return summed.reshape(out_width, inner_x, inner_y, depth_z)


def gradients(padded):
    center = padded[:, 1:-1, 1:-1]
    diff_x = (padded[:, 2:, 1:-1] - padded[:, :-2, 1:-1]) * 0.5
    diff_y = (padded[:, 1:-1, 2:] - padded[:, 1:-1, :-2]) * 0.5
    diff_z = (jnp.roll(center, -1, axis=3) - jnp.roll(center, 1, axis=3)) * 0.5
    stacked = jnp.stack([diff_x, diff_y, diff_z], axis=1)
    return stacked.reshape((9,) + center.shape[1:])


def laplace(padded):
    center = padded[:, 1:-1, 1:-1]
    beside_all = padded[:, 2:, 1:-1] + padded[:, :-2, 1:-1] + padded[:, 1:-1, 2:] + padded[:, 1:-1, :-2]
    beside_all = beside_all + jnp.roll(center, 1, axis=3) + jnp.roll(center, -1, axis=3)
    return beside_all - 6.0 * center


def spread(padded):
    center = padded[:, 1:-1, 1:-1]
    diff_x = (padded[:, 2:, 1:-1] - padded[:, :-2, 1:-1]) * 0.5
    diff_y = (padded[:, 1:-1, 2:] - padded[:, 1:-1, :-2]) * 0.5
    diff_z = (jnp.roll(center, -1, axis=3) - jnp.roll(center, 1, axis=3)) * 0.5
    return jnp.stack([diff_x[pairing[component][0]] + diff_y[pairing[component][1]] + diff_z[pairing[component][2]] for component in range(3)])


def advance(velocity, grads, laplacian, divergence, forcing):
    advect = jnp.sum(grads.reshape((3, 3) + grads.shape[1:]) * velocity[None], axis=1)
    tendency = -advect + viscosity * laplacian - divergence + forcing * velocity
    return velocity + time_step * tendency


def wrap_pad(source, margin):
    return jnp.pad(source, ((0, 0), (margin, margin), (margin, margin), (0, 0)), mode="wrap")


def activate(summed):
    return jnp.tanh(summed).astype(jnp.bfloat16)


def unchanged(summed):
    return summed


def conv_full(source, weight, offset, finish):
    padded = wrap_pad(source, 1)
    block_count = NX // CX

    def one_block(block_id):
        window = lax.dynamic_slice_in_dim(padded, block_id * CX, CX + 2, 1)
        return finish(convolve(window, weight, offset))

    result = lax.map(one_block, jnp.arange(block_count, dtype=jnp.int32))
    result = jnp.transpose(result, (1, 0, 2, 3, 4))
    return result.reshape(result.shape[0], NX, NY, NZ)


def reference(velocity, first_weight, first_bias, second_weight, second_bias, third_weight, third_bias, last_weight):
    padded = wrap_pad(velocity, 1)
    grads = gradients(padded)
    laplacian = laplace(padded)
    features = grads.astype(jnp.bfloat16)
    layer_one = conv_full(features, first_weight, first_bias, activate)
    layer_two = conv_full(layer_one, second_weight, second_bias, activate)
    layer_three = conv_full(layer_two, third_weight, third_bias, activate)
    stress = conv_full(layer_three, last_weight, jnp.zeros((6,), jnp.float32), unchanged)
    divergence = spread(wrap_pad(stress, 1))
    energy = jnp.mean(0.5 * jnp.sum(velocity * velocity, axis=0))
    forcing = power_input / (2.0 * energy + 1e-6)
    updated = advance(velocity, grads, laplacian, divergence, forcing)
    return updated, stress
```

```python
import functools

import jax
import jax.numpy as jnp
from jax import lax
from jax.experimental import pallas as pl
from jax.experimental.pallas import tpu as pltpu
from jax.sharding import PartitionSpec as P

time_step = 0.1
viscosity = 0.05
power_input = 5.0
pairing = ((0, 3, 4), (3, 1, 5), (4, 5, 2))
halo = 6
axis_x = ("grp", "gx")
axis_y = "gy"
slot = 32
f32 = jnp.float32
bf16 = jnp.bfloat16


def shifted(cells, axis, step):
    count = lax.axis_size(axis)
    return lax.ppermute(cells, axis, [(i, (i + step) % count) for i in range(count)])


def neighbours(cells, axis, dim):
    extent = cells.shape[dim]
    before, after = [], []
    hop, need = 1, halo
    while need > 0:
        width = min(extent, need)
        tail = lax.slice_in_dim(cells, extent - width, extent, axis=dim)
        head = lax.slice_in_dim(cells, 0, width, axis=dim)
        before.insert(0, shifted(tail, axis, hop))
        after.append(shifted(head, axis, -hop))
        hop += 1
        need -= width
    return before, after


def blocks_in(extent, count):
    size = 1
    while count % (2 * size) == 0 and 2 * size * extent <= extent + 2 * halo:
        size *= 2
    return size


def pair_rows(get, xin, xout):
    parts = []
    for xo in range(xout):
        parts.append(get(xin - xo) if 0 <= xin - xo <= 2 else None)
    return parts


def expand_hidden(w_ref, out_ref):
    channels = w_ref.shape[3]
    outs = w_ref.shape[4 - 1]
    zero = jnp.zeros((outs, channels), f32)
    blank = jnp.zeros((channels, 2 * outs), bf16)
    for dz in range(3):
        for xin in range(4):
            tall = []
            for dy in range(3):
                rows = [
                    w_ref[xin - xo, dy, dz].astype(f32) if 0 <= xin - xo <= 2 else zero
                    for xo in range(2)
                ]
                tall.append(jnp.concatenate(rows, axis=0).T.astype(bf16))
            for yin in range(4):
                base = ((dz * 4 + yin) * 4 + xin) * channels
                for yo in range(2):
                    piece = tall[yin - yo] if 0 <= yin - yo <= 2 else blank
                    out_ref[base : base + channels, yo * 2 * outs : (yo + 1) * 2 * outs] = piece


def expand_first(w_ref, out_ref):
    outs, inner = w_ref.shape[3], w_ref.shape[4]
    fill = slot - 3 * inner
    zero = jnp.zeros((outs, slot), f32)
    blank = jnp.zeros((slot, 2 * outs), bf16)
    flat = {}
    for dx in range(3):
        for dy in range(3):
            parts = [w_ref[dx, dy, dz].astype(f32) for dz in range(3)]
            parts.append(jnp.zeros((outs, fill), f32))
            flat[dx, dy] = jnp.concatenate(parts, axis=1)
    for xin in range(4):
        tall = []
        for dy in range(3):
            rows = [flat[xin - xo, dy] if 0 <= xin - xo <= 2 else zero for xo in range(2)]
            tall.append(jnp.concatenate(rows, axis=0).T.astype(bf16))
        for yin in range(4):
            base = (xin * 4 + yin) * slot
            for yo in range(2):
                piece = tall[yin - yo] if 0 <= yin - yo <= 2 else blank
                out_ref[base : base + slot, yo * 2 * outs : (yo + 1) * 2 * outs] = piece


def expand_last(w_ref, out_ref):
    outs, channels = w_ref.shape[3], w_ref.shape[4]
    zero = jnp.zeros((8, channels), f32)
    pad = jnp.zeros((8 - outs, channels), f32)
    taps = {}
    for dx in range(3):
        for dy in range(3):
            for dz in range(3):
                taps[dx, dy, dz] = jnp.concatenate([w_ref[dx, dy, dz].astype(f32), pad], axis=0)
    for yin in range(4):
        for pair in range(2):
            column = []
            for dz in range(3):
                for yo in range(2):
                    for xo in range(2):
                        halves = []
                        for xin in (2 * pair, 2 * pair + 1):
                            dx, dy = xin - xo, yin - yo
                            inside = 0 <= dx <= 2 and 0 <= dy <= 2
                            halves.append(taps[dx, dy, dz] if inside else zero)
                        column.append(jnp.concatenate(halves, axis=1))
            base = (yin * 2 + pair) * 2 * channels
            out_ref[:, base : base + 2 * channels] = jnp.concatenate(column, axis=0).astype(bf16)


def prepare_kernel(w1, w2, w3, w4, o1, o2, o3, o4):
    expand_first(w1, o1)
    expand_hidden(w2, o2)
    expand_hidden(w3, o3)
    expand_last(w4, o4)


def prepare(w1, w2, w3, w4):
    outs, channels = w2.shape[3], w2.shape[4]
    vmem = pl.BlockSpec(memory_space=pltpu.VMEM)
    return pl.pallas_call(
        prepare_kernel,
        out_shape=(
            jax.ShapeDtypeStruct((16 * slot, 4 * outs), bf16),
            jax.ShapeDtypeStruct((48 * channels, 4 * outs), bf16),
            jax.ShapeDtypeStruct((48 * channels, 4 * outs), bf16),
            jax.ShapeDtypeStruct((96, 16 * channels), bf16),
        ),
        in_specs=[vmem] * 4,
        out_specs=(vmem,) * 4,
        cost_estimate=pl.CostEstimate(flops=10**9, bytes_accessed=8 * 10**6, transcendentals=0),
        compiler_params=pltpu.CompilerParams(vmem_limit_bytes=24 * 2**20),
        name="prepare",
    )(w1, w2, w3, w4)


def main_kernel(count, *refs):
    pieces = refs[:count]
    (w1, b1, w2, b2, w3, b3, w4) = refs[count : count + 7]
    base_ref, stress_ref = refs[count + 7 : count + 9]
    vel, feat, turned, h1, h2, h3, tau = refs[count + 9 :]
    depth = vel.shape[3]
    wide_x, wide_y = vel.shape[1], vel.shape[2]
    fx, fy = wide_x - 2, wide_y - 2

    at = 0
    for piece in pieces:
        vel[:, at : at + piece.shape[1]] = piece[...]
        at += piece.shape[1]

    feat[...] = jnp.zeros_like(feat)

    def features(x, carry):
        for i in range(3):
            row = vel[i, x + 1]
            center = row[1:-1]
            diffs = (
                (vel[i, x + 2][1:-1] - vel[i, x][1:-1]) * 0.5,
                (row[2:] - row[:-2]) * 0.5,
                (pltpu.roll(center, depth - 1, 1) - pltpu.roll(center, 1, 1)) * 0.5,
            )
            for j in range(3):
                value = diffs[j].astype(bf16).astype(f32)
                for dz, amount in enumerate((1, 0, depth - 1)):
                    moved = pltpu.roll(value, amount, 1) if amount else value
                    feat[pl.ds(dz * 9 + 3 * i + j, fy, stride=slot), :] = moved
        for half in range(fy // 2 - 1):
            block = feat[half * 2 * slot : half * 2 * slot + 4 * slot, :]
            turned[x, half] = block.astype(bf16).T
        return carry

    lax.fori_loop(0, fx, features, 0)

    def layer(gather, weight, bias_ref, target, steps, variants):
        bias = jnp.concatenate([bias_ref[...]] * 4, axis=1)

        def step(xp, carry):
            left = gather(xp)
            total = jnp.dot(left, weight[...], preferred_element_type=f32)
            value = jnp.tanh(total + bias)
            rows = value.shape[0] // depth
            value = value.reshape(rows, depth, value.shape[1])
            width = value.shape[2] // 2
            for dz, amount in enumerate((1, 0, depth - 1)):
                if dz not in variants:
                    continue
                moved = pltpu.roll(value, amount, 1) if amount else value
                moved = moved.astype(bf16)
                for yo in range(2):
                    where = (xp, yo) if len(variants) == 1 else (dz, xp, yo)
                    target[where] = moved[:, :, yo * width : (yo + 1) * width]
            return carry

        lax.fori_loop(0, steps, step, 0)

    def gather_first(xp):
        parts = []
        for a in range(4):
            block = turned[2 * xp + a]
            parts.append(block.reshape(block.shape[0] * block.shape[1], block.shape[2]))
        return jnp.concatenate(parts, axis=1)

    def gather_hidden(source, variants):
        rows = source.shape[-3] - 1

        def gather(xp):
            parts = []
            for dz in variants:
                for yin in range(4):
                    for pair in range(2):
                        where = (xp + pair, yin % 2, slice(yin // 2, yin // 2 + rows))
                        block = source[where if len(source.shape) == 5 else (dz, *where)]
                        parts.append(block.reshape(rows * block.shape[1], block.shape[2]))
            return jnp.concatenate(parts, axis=1)

        return gather

    every = (0, 1, 2)
    layer(gather_first, w1, b1, h1, h1.shape[1], every)
    layer(gather_hidden(h1, every), w2, b2, h2, h2.shape[1], every)
    layer(gather_hidden(h2, every), w3, b3, h3, h3.shape[0], (1,))

    last = gather_hidden(h3, (1,))

    def final(xp, carry):
        sides = lax.dot_general(
            w4[...], last(xp), (((1,), (1,)), ((), ())), preferred_element_type=f32
        )
        for yp in range(sides.shape[1] // depth):
            part = sides[:, yp * depth : (yp + 1) * depth]
            total = pltpu.roll(part[0:32], 1, 1) + part[32:64] + pltpu.roll(part[64:96], depth - 1, 1)
            for yo in range(2):
                for xo in range(2):
                    cell = (2 * yo + xo) * 8
                    row = (2 * yp + yo) * 8
                    tau[2 * xp + xo, row : row + 8, :] = total[cell : cell + 8]
        return carry

    lax.fori_loop(0, h3.shape[0] - 1, final, 0)

    own_x, own_y = base_ref.shape[1], base_ref.shape[2]

    def stress_at(c, x, y):
        return tau[x, pl.ds(y * 8 + c, own_y, stride=8), :]

    def turn(a, amount):
        return pltpu.roll(a, amount % depth, 1)

    for x in range(own_x):
        for c in range(6):
            stress_ref[c, x] = stress_at(c, x + 1, 1)
        center = [vel[i, x + halo, halo : halo + own_y, :] for i in range(3)]
        for i in range(3):
            xm = vel[i, x + halo - 1, halo : halo + own_y, :]
            xp = vel[i, x + halo + 1, halo : halo + own_y, :]
            ym = vel[i, x + halo, halo - 1 : halo - 1 + own_y, :]
            yp = vel[i, x + halo, halo + 1 : halo + 1 + own_y, :]
            zm, zp = turn(center[i], 1), turn(center[i], -1)
            advect = (
                center[0] * ((xp - xm) * 0.5)
                + center[1] * ((yp - ym) * 0.5)
                + center[2] * ((zp - zm) * 0.5)
            )
            laplacian = xp + xm + yp + ym + zm + zp - 6.0 * center[i]
            px, py, pz = pairing[i]
            along_z = stress_at(pz, x + 1, 1)
            divergence = (
                (stress_at(px, x + 2, 1) - stress_at(px, x, 1)) * 0.5
                + (stress_at(py, x + 1, 2) - stress_at(py, x + 1, 0)) * 0.5
                + (turn(along_z, -1) - turn(along_z, 1)) * 0.5
            )
            tendency = viscosity * laplacian - advect - divergence
            base_ref[i, x] = center[i] + time_step * tendency


def evolve(velocity, pieces, weights):
    parts, own_x, own_y, depth = velocity.shape
    w1, b1, w2, b2, w3, b3, w4 = weights
    width = 2 * b1.shape[1]
    wide_x, wide_y = own_x + 2 * halo, own_y + 2 * halo
    qx, qy = (wide_x - 4) // 2, (wide_y - 4) // 2
    vmem = pl.BlockSpec(memory_space=pltpu.VMEM)
    stress_count = 6
    cells1 = 4 * qx * qy * depth
    flops = 2 * depth * 256 * (qx * qy * 512 + (qx - 1) * (qy - 1) * 3072 + (qx - 2) * (qy - 2) * 3072)
    return pl.pallas_call(
        functools.partial(main_kernel, len(pieces)),
        out_shape=(
            jax.ShapeDtypeStruct(velocity.shape, f32),
            jax.ShapeDtypeStruct((stress_count,) + velocity.shape[1:], f32),
        ),
        in_specs=[vmem] * (len(pieces) + 7),
        out_specs=(vmem, vmem),
        scratch_shapes=[
            pltpu.VMEM((parts, wide_x, wide_y, depth), f32),
            pltpu.VMEM(((wide_y - 2) * slot, depth), f32),
            pltpu.VMEM((wide_x - 2, qy, depth, 4 * slot), bf16),
            pltpu.VMEM((3, qx, 2, qy, depth, width), bf16),
            pltpu.VMEM((3, qx - 1, 2, qy - 1, depth, width), bf16),
            pltpu.VMEM((qx - 2, 2, qy - 2, depth, width), bf16),
            pltpu.VMEM((wide_x - 10, (wide_y - 10) * 8, depth), f32),
        ],
        cost_estimate=pl.CostEstimate(
            flops=flops, bytes_accessed=8 * 10**6, transcendentals=cells1 * 64
        ),
        compiler_params=pltpu.CompilerParams(vmem_limit_bytes=44 * 2**20),
        name="evolve",
    )(*pieces, *weights)


def box_energy(pieces, own_x, own_y, count_x, count_y):
    wide_y = pieces[0].shape[2]
    span_x, span_y = count_x * own_x, count_y * own_y
    low_x = (own_x + 2 * halo - span_x) // 2
    low_y = (wide_y - span_y) // 2
    total, at = None, 0
    for piece in pieces:
        low, high = max(low_x - at, 0), min(low_x + span_x - at, piece.shape[1])
        if low < high:
            part = piece[:, low:high, low_y : low_y + span_y]
            part = jnp.sum(0.5 * part * part, axis=(0, 1, 2))
            total = part if total is None else total + part
        at += piece.shape[1]
    return jnp.sum(total, keepdims=True).reshape(1, 1) * jnp.ones((1, 128), f32)


def total_energy(box, size_x, size_y):
    count_x, count_y = lax.axis_size(axis_x), lax.axis_size(axis_y)
    left_x, left_y = count_x // size_x, count_y // size_y
    if (left_x & (left_x - 1)) or (left_y & (left_y - 1)):
        return lax.psum(box, axis_x + (axis_y,)) / (size_x * size_y)
    step = size_x
    while left_x > 2:
        box = box + shifted(box, axis_x, step)
        step, left_x = 2 * step, left_x // 2
    hop = size_y
    while left_y > 2:
        box = box + shifted(box, axis_y, hop)
        hop, left_y = 2 * hop, left_y // 2
    total = box
    if left_x == 2:
        total = total + shifted(box, axis_x, step)
    if left_y == 2:
        total = total + shifted(box, axis_y, hop)
    if left_x == 2 and left_y == 2:
        order = [
            (
                x * count_y + y,
                ((x + step) % count_x) * count_y + (y + hop) % count_y,
            )
            for x in range(count_x)
            for y in range(count_y)
        ]
        total = total + lax.ppermute(box, axis_x + (axis_y,), order)
    return total


def local(v, w1, b1, w2, b2, w3, b3, w4):
    own_x, own_y, depth = v.shape[1:]
    count_x, count_y = lax.axis_size(axis_x), lax.axis_size(axis_y)
    e1, e2, e3, e4 = prepare(w1, w2, w3, w4)
    before, after = neighbours(v, axis_y, 2)
    strip = jnp.concatenate(before + [v] + after, axis=2)
    before, after = neighbours(strip, axis_x, 1)
    pieces = before + [strip] + after
    size_x, size_y = blocks_in(own_x, count_x), blocks_in(own_y, count_y)
    box = box_energy(pieces, own_x, own_y, size_x, size_y)
    energy = total_energy(box, size_x, size_y)[0, 0]
    energy = energy / (own_x * own_y * depth * count_x * count_y)
    forcing = power_input / (2.0 * energy + 1e-06)
    weights = (e1, b1.reshape(1, -1), e2, b2.reshape(1, -1), e3, b3.reshape(1, -1), e4)
    base, stress = evolve(v, pieces, weights)
    return base + (time_step * forcing) * v, stress


def solution(mesh):
    block = P(None, axis_x, axis_y, None)
    return jax.shard_map(
        local,
        mesh=mesh,
        in_specs=(block,) + (P(),) * 7,
        out_specs=(block, block),
        check_vma=False,
    )
```

```python
import functools

import jax
import jax.numpy as jnp
from jax import lax
from jax.experimental import pallas as pl
from jax.experimental.pallas import tpu as pltpu
from jax.sharding import PartitionSpec as P

time_step = 0.1
viscosity = 0.05
power_input = 5.0
pairing = ((0, 3, 4), (3, 1, 5), (4, 5, 2))
halo = 6
axis_x = ("grp", "gx")
axis_y = "gy"
groups = 8
f32 = jnp.float32
bf16 = jnp.bfloat16


def shifted(cells, axis, step):
    count = lax.axis_size(axis)
    return lax.ppermute(cells, axis, [(i, (i + step) % count) for i in range(count)])


def neighbours(cells, axis, dim):
    extent = cells.shape[dim]
    before, after = [], []
    hop, need = 1, halo
    while need > 0:
        width = min(extent, need)
        tail = lax.slice_in_dim(cells, extent - width, extent, axis=dim)
        head = lax.slice_in_dim(cells, 0, width, axis=dim)
        before.insert(0, shifted(tail, axis, hop))
        after.append(shifted(head, axis, -hop))
        hop += 1
        need -= width
    return before, after


def blocks_in(extent, count):
    size = 1
    while count % (2 * size) == 0 and 2 * size * extent <= extent + 2 * halo:
        size *= 2
    return size


def expand_hidden(w_ref, out_ref):
    outs, channels = w_ref.shape[3], w_ref.shape[4]
    zero = jnp.zeros((outs, channels), f32)
    blank = jnp.zeros((channels, 2 * outs), bf16)
    for dz in range(3):
        for xin in range(4):
            tall = []
            for dy in range(3):
                rows = [
                    w_ref[xin - xo, dy, dz].astype(f32) if 0 <= xin - xo <= 2 else zero
                    for xo in range(2)
                ]
                tall.append(jnp.concatenate(rows, axis=0).T.astype(bf16))
            for yin in range(4):
                base = ((dz * 4 + yin) * 4 + xin) * channels
                for yo in range(2):
                    piece = tall[yin - yo] if 0 <= yin - yo <= 2 else blank
                    out_ref[base : base + channels, yo * 2 * outs : (yo + 1) * 2 * outs] = piece


def selector(yo):
    row = lax.broadcasted_iota(jnp.int32, (128, 128), 0)
    column = lax.broadcasted_iota(jnp.int32, (128, 128), 1)
    group, yin, part = row >> 4, (row >> 2) & 3, row & 3
    one, two = jnp.where(group >= 3, 1, 0), jnp.where(group >= 6, 1, 0)
    along = one + two
    dz = group - 3 * along
    spare = part == 3
    along = jnp.where(spare, 2, along)
    dz = jnp.where(spare, 2, dz)
    part = jnp.where(spare, group, part)
    wanted = (yin - yo) * 32 + (3 * part + along) * 3 + dz
    fits = (yin >= yo) & (yin - yo <= 2) & (part <= 2) & (column == wanted)
    return jnp.where(fits, 1.0, 0.0).astype(bf16)


def expand_first(w_ref, out_ref, flat):
    features, outs = w_ref.shape[2], w_ref.shape[4]
    flat[...] = jnp.zeros_like(flat)
    for dx in range(3):
        for dy in range(3):
            for channel in range(features):
                row = dy * 32 + channel * 3
                flat[dx, row : row + 3, :] = w_ref[dx, dy, channel].astype(f32)
    zero = jnp.zeros(flat.shape[1:], f32)
    for yo in range(2):
        pick = selector(yo)
        for xin in range(4):
            sides = [flat[xin - xo] if 0 <= xin - xo <= 2 else zero for xo in range(2)]
            both = jnp.concatenate(sides, axis=1).astype(bf16)
            block = jnp.dot(pick, both, preferred_element_type=f32)
            out_ref[xin * 128 : (xin + 1) * 128, yo * 2 * outs : (yo + 1) * 2 * outs] = (
                block.astype(bf16)
            )


def expand_last(w_ref, out_ref):
    outs, channels = w_ref.shape[3], w_ref.shape[4]
    zero = jnp.zeros((8, channels), f32)
    pad = jnp.zeros((8 - outs, channels), f32)
    taps = {}
    for dx in range(3):
        for dy in range(3):
            for dz in range(3):
                taps[dx, dy, dz] = jnp.concatenate([w_ref[dx, dy, dz].astype(f32), pad], axis=0)
    for yin in range(4):
        for pair in range(2):
            column = []
            for dz in range(3):
                for yo in range(2):
                    for xo in range(2):
                        halves = []
                        for xin in (2 * pair, 2 * pair + 1):
                            dx, dy = xin - xo, yin - yo
                            inside = 0 <= dx <= 2 and 0 <= dy <= 2
                            halves.append(taps[dx, dy, dz] if inside else zero)
                        column.append(jnp.concatenate(halves, axis=1))
            base = (yin * 2 + pair) * 2 * channels
            out_ref[:, base : base + 2 * channels] = jnp.concatenate(column, axis=0).astype(bf16)


def first_kernel(w1, b1, out_ref, bias, flat):
    bias[...] = jnp.concatenate([b1[...]] * 4, axis=1)
    expand_first(w1, out_ref, flat)


def later_kernel(w2, w3, w4, o2, o3, o4):
    expand_hidden(w2, o2)
    expand_hidden(w3, o3)
    expand_last(w4, o4)


def ends_kernel(width, v, head, tail):
    extent = v.shape[2]
    head[...] = v[:, :, 0:width, :]
    tail[...] = v[:, :, extent - width : extent, :]


def whole():
    return pl.BlockSpec(memory_space=pltpu.VMEM)


def granted(mib):
    return pltpu.CompilerParams(vmem_limit_bytes=mib * 2**20)


def priced(flops):
    return pl.CostEstimate(flops=int(flops), bytes_accessed=10**6, transcendentals=0)


def ends(v, width):
    shape = jax.ShapeDtypeStruct(v.shape[:2] + (width,) + v.shape[3:], f32)
    return pl.pallas_call(
        functools.partial(ends_kernel, width),
        out_shape=(shape, shape),
        in_specs=[whole()],
        out_specs=(whole(), whole()),
        compiler_params=granted(4),
        name="ends",
    )(v)


def prepare_first(w1, b1):
    outs = w1.shape[3]
    w1 = jnp.transpose(w1, (0, 1, 4, 2, 3))
    return pl.pallas_call(
        first_kernel,
        out_shape=(
            jax.ShapeDtypeStruct((512, 4 * outs), bf16),
            jax.ShapeDtypeStruct((1, 4 * outs), f32),
        ),
        in_specs=[whole()] * 2,
        out_specs=(whole(),) * 2,
        scratch_shapes=[pltpu.VMEM((3, 128, outs), f32)],
        cost_estimate=pl.CostEstimate(flops=4 * 10**9, bytes_accessed=10**7, transcendentals=0),
        compiler_params=granted(10),
        name="prepare_first",
    )(w1, b1.reshape(1, -1))


def prepare_later(w2, w3, w4):
    outs, channels = w2.shape[3], w2.shape[4]
    return pl.pallas_call(
        later_kernel,
        out_shape=(
            jax.ShapeDtypeStruct((48 * channels, 4 * outs), bf16),
            jax.ShapeDtypeStruct((48 * channels, 4 * outs), bf16),
            jax.ShapeDtypeStruct((96, 16 * channels), bf16),
        ),
        in_specs=[whole()] * 3,
        out_specs=(whole(),) * 3,
        cost_estimate=priced(10**9),
        compiler_params=granted(10),
        name="prepare_later",
    )(w2, w3, w4)


def lay_rows(target, at, piece, x):
    count = piece.shape[2]
    for c in range(3):
        target[at, pl.ds(c, count, stride=4), :] = piece[c, x]
    target[at, pl.ds(3, count, stride=4), :] = jnp.zeros((count, piece.shape[3]), f32)


def features(rows, at, depth):
    total = rows.shape[1]
    center = rows[at + 1, 4 : total - 4, :]
    diffs = (
        (rows[at + 2, 4 : total - 4, :] - rows[at, 4 : total - 4, :]) * 0.5,
        (rows[at + 1, 8:total, :] - rows[at + 1, 0 : total - 8, :]) * 0.5,
        (pltpu.roll(center, depth - 1, 1) - pltpu.roll(center, 1, 1)) * 0.5,
    )
    parts = []
    for j in range(3):
        for amount in (1, 0, depth - 1):
            parts.append(pltpu.roll(diffs[j], amount, 1) if amount else diffs[j])
    spare = parts.pop()
    lane = lax.broadcasted_iota(jnp.int32, spare.shape, 0) & 3
    for c in range(3):
        parts[c] = jnp.where(lane == 3, pltpu.roll(spare, 3 - c, 0), parts[c])
    turned = []
    for half in range((total // 4 - 2) // 2 - 1):
        block = jnp.concatenate([part[8 * half : 8 * half + 16] for part in parts], axis=0)
        turned.append(block.astype(bf16).T)
    return turned


def merge(block):
    return block.reshape(block.shape[0] * block.shape[1], block.shape[2])


def layer(left, weight, bias, store, depth, variants):
    total = jnp.dot(left, weight[...], preferred_element_type=f32)
    value = jnp.tanh(total + bias)
    value = value.reshape(value.shape[0] // depth, depth, value.shape[1])
    width = value.shape[2] // 2
    for dz, amount in enumerate((1, 0, depth - 1)):
        if dz not in variants:
            continue
        moved = pltpu.roll(value, amount, 1) if amount else value
        moved = moved.astype(bf16)
        for yo in range(2):
            store(dz, yo, moved[:, :, yo * width : (yo + 1) * width])


every = (0, 1, 2)


def gather_hidden(source, xp, variants):
    rows = source.shape[-3] - 1
    parts = []
    for dz in variants:
        for yin in range(4):
            for pair in range(2):
                where = (xp + pair, yin % 2, slice(yin // 2, yin // 2 + rows))
                parts.append(merge(source[where if len(source.shape) == 5 else (dz, *where)]))
    return jnp.concatenate(parts, axis=1)


def store_hidden(target, xp):
    def store(dz, yo, block):
        target[(xp, yo) if len(target.shape) == 5 else (dz, xp, yo)] = block

    return store


def inner_kernel(low, near, own, far, w1, bias, h1, turned, rows):
    depth = own.shape[3]
    at = 0
    for piece in (near, own, far):
        for x in range(piece.shape[1]):
            lay_rows(rows, at, piece, x)
            at += 1

    def one(x, carry):
        for half, block in enumerate(features(rows, x, depth)):
            turned[x, half] = block
        return carry

    lax.fori_loop(0, turned.shape[0], one, 0, unroll=2)

    def step(q, carry):
        left = jnp.concatenate([merge(turned[2 * q + a]) for a in range(4)], axis=1)
        layer(left, w1, bias[...], store_hidden(h1, q + low), depth, every)
        return carry

    lax.fori_loop(0, turned.shape[0] // 2 - 1, step, 0)


def outer_kernel(count, box, *refs):
    pieces = refs[:count]
    turned, w1, bias, _, h1, energy, rows, edges = refs[count:]
    depth = pieces[0].shape[3]
    columns = [(piece, x) for piece in pieces for x in range(piece.shape[1])]
    need = rows.shape[1]
    edge = need - 2
    for side, part in enumerate((columns[:need], columns[-need:])):
        for at, (piece, x) in enumerate(part):
            lay_rows(rows.at[side], at, piece, x)
        for at in range(edge):
            for half, block in enumerate(features(rows.at[side], at, depth)):
                edges[side, at, half] = block
    inside = turned.shape[0]
    held = [edges.at[0, k] for k in range(edge)] + [turned.at[k] for k in range(inside)]
    held += [edges.at[1, k] for k in range(edge)]
    pairs = h1.shape[1]
    for k in range(edge // 2):
        for xp in (k, pairs - 1 - k):
            left = jnp.concatenate([merge(held[2 * xp + a][...]) for a in range(4)], axis=1)
            layer(left, w1, bias[...], store_hidden(h1, xp), depth, every)
    low_x, span_x, low_y, span_y = box
    total = None
    for piece, x in columns[low_x : low_x + span_x]:
        for c in range(3):
            part = piece[c, x, low_y : low_y + span_y, :]
            total = part * part if total is None else total + part * part
    energy[...] = jnp.broadcast_to(0.5 * jnp.sum(total, keepdims=True), energy.shape)


def second_kernel(h1, w2, bias, h2):
    depth = h1.shape[4]

    def step(xp, carry):
        layer(gather_hidden(h1, xp, every), w2, jnp.concatenate([bias[...]] * 4, axis=1), store_hidden(h2, xp), depth, every)
        return carry

    lax.fori_loop(0, h2.shape[1], step, 0)


def third_kernel(h2, w3, bias, h3):
    depth = h2.shape[4]

    def step(xp, carry):
        layer(gather_hidden(h2, xp, every), w3, jnp.concatenate([bias[...]] * 4, axis=1), store_hidden(h3, xp), depth, (1,))
        return carry

    lax.fori_loop(0, h3.shape[0], step, 0)


def final_kernel(cells, h3, w4, near, own, far, energy, updated_ref, stress_ref, tau):
    depth = own.shape[3]
    forcing = power_input / (2.0 * (energy[0, 0] / cells) + 1e-06)

    def final(xp, carry):
        sides = lax.dot_general(
            w4[...],
            gather_hidden(h3, xp, (1,)),
            (((1,), (1,)), ((), ())),
            preferred_element_type=f32,
        )
        for yp in range(sides.shape[1] // depth):
            part = sides[:, yp * depth : (yp + 1) * depth]
            total = pltpu.roll(part[0:32], 1, 1) + part[32:64] + pltpu.roll(part[64:96], depth - 1, 1)
            for yo in range(2):
                for xo in range(2):
                    cell = (2 * yo + xo) * 8
                    row = (2 * yp + yo) * 8
                    tau[2 * xp + xo, row : row + 8, :] = total[cell : cell + 8]
        return carry

    lax.fori_loop(0, h3.shape[0] - 1, final, 0)

    own_x, own_y = updated_ref.shape[1], updated_ref.shape[2]

    def stress_at(c, x, y):
        return tau[x, pl.ds(y * 8 + c, own_y, stride=8), :]

    def turn(a, amount):
        return pltpu.roll(a, amount % depth, 1)

    def vel(i, x, y):
        piece, at = own, x
        if x < 0:
            piece, at = near, x + near.shape[1]
        elif x >= own_x:
            piece, at = far, x - own_x
        return piece[i, at, halo + y : halo + y + own_y, :]

    for x in range(own_x):
        for c in range(6):
            stress_ref[c, x] = stress_at(c, x + 1, 1)
        center = [vel(i, x, 0) for i in range(3)]
        for i in range(3):
            xm, xp, ym, yp = vel(i, x - 1, 0), vel(i, x + 1, 0), vel(i, x, -1), vel(i, x, 1)
            zm, zp = turn(center[i], 1), turn(center[i], -1)
            advect = (
                center[0] * ((xp - xm) * 0.5)
                + center[1] * ((yp - ym) * 0.5)
                + center[2] * ((zp - zm) * 0.5)
            )
            laplacian = xp + xm + yp + ym + zm + zp - 6.0 * center[i]
            px, py, pz = pairing[i]
            along_z = stress_at(pz, x + 1, 1)
            divergence = (
                (stress_at(px, x + 2, 1) - stress_at(px, x, 1)) * 0.5
                + (stress_at(py, x + 1, 2) - stress_at(py, x + 1, 0)) * 0.5
                + (turn(along_z, -1) - turn(along_z, 1)) * 0.5
            )
            tendency = viscosity * laplacian - advect - divergence + forcing * center[i]
            updated_ref[i, x] = center[i] + time_step * tendency


def box_total(box, size_x, size_y):
    count_x, count_y = lax.axis_size(axis_x), lax.axis_size(axis_y)
    left_x, left_y = count_x // size_x, count_y // size_y
    if (left_x & (left_x - 1)) or (left_y & (left_y - 1)):
        return lax.psum(box, axis_x + (axis_y,)) / (size_x * size_y)
    while size_x < count_x:
        box = box + shifted(box, axis_x, size_x)
        size_x *= 2
    while size_y < count_y:
        box = box + shifted(box, axis_y, size_y)
        size_y *= 2
    return box


def local(v, w1, b1, w2, b2, w3, b3, w4):
    parts, own_x, own_y, depth = v.shape
    count_x, count_y = lax.axis_size(axis_x), lax.axis_size(axis_y)
    width = 2 * w2.shape[3]
    bias2, bias3 = b2.reshape(1, -1), b3.reshape(1, -1)
    if own_y >= halo:
        head, tail = ends(v, halo)
        before, after = [shifted(tail, axis_y, 1)], [shifted(head, axis_y, -1)]
    else:
        before, after = neighbours(v, axis_y, 2)
    e1, bias1 = prepare_first(w1, b1)
    strip = jnp.concatenate(before + [v] + after, axis=2)
    w2, w3, w4, strip = lax.optimization_barrier((w2, w3, w4, strip))
    e2, e3, e4 = prepare_later(w2, w3, w4)
    before, after = neighbours(strip, axis_x, 1)
    near, far = before[-1], after[0]
    pieces = before + [strip] + after

    wide_x, wide_y = own_x + 2 * halo, own_y + 2 * halo
    qx, qy = (wide_x - 4) // 2, (wide_y - 4) // 2
    edge = halo - near.shape[1]
    inside = wide_x - 2 - 2 * edge
    h1_shape = jax.ShapeDtypeStruct((3, qx, 2, qy, depth, width), bf16)
    h2_shape = jax.ShapeDtypeStruct((3, qx - 1, 2, qy - 1, depth, width), bf16)

    tile = 2 * depth * 256 * 256
    h1, turned = pl.pallas_call(
        functools.partial(inner_kernel, edge // 2),
        out_shape=(h1_shape, jax.ShapeDtypeStruct((inside, qy, depth, 128), bf16)),
        in_specs=[whole()] * 5,
        out_specs=(whole(), whole()),
        scratch_shapes=[pltpu.VMEM((inside + 2, 4 * wide_y, depth), f32)],
        cost_estimate=priced(4 * tile * qx * qy),
        compiler_params=granted(12),
        name="inner",
    )(near, strip, far, e1, bias1)

    size_x, size_y = blocks_in(own_x, count_x), blocks_in(own_y, count_y)
    box = (
        (wide_x - size_x * own_x) // 2,
        size_x * own_x,
        (wide_y - size_y * own_y) // 2,
        size_y * own_y,
    )
    count = len(pieces)
    h1, energy = pl.pallas_call(
        functools.partial(outer_kernel, count, box),
        out_shape=(h1_shape, jax.ShapeDtypeStruct((1, 1, 1, depth), f32)),
        in_specs=[whole()] * (count + 4),
        out_specs=(whole(), whole()),
        scratch_shapes=[
            pltpu.VMEM((2, edge + 2, 4 * wide_y, depth), f32),
            pltpu.VMEM((2, edge, qy, depth, 128), bf16),
        ],
        input_output_aliases={count + 3: 0},
        cost_estimate=priced(2 * tile * qx * qy),
        compiler_params=granted(12),
        name="outer",
    )(*pieces, turned, e1, bias1, h1)

    h2 = pl.pallas_call(
        second_kernel,
        out_shape=h2_shape,
        in_specs=[whole()] * 3,
        out_specs=whole(),
        cost_estimate=priced(12 * tile * (qx - 1) * (qy - 1)),
        compiler_params=granted(20),
        name="second",
    )(h1, e2, bias2)

    energy = box_total(energy, size_x, size_y)
    cells = own_x * own_y * depth * count_x * count_y

    h3 = pl.pallas_call(
        third_kernel,
        out_shape=jax.ShapeDtypeStruct((qx - 2, 2, qy - 2, depth, width), bf16),
        in_specs=[whole()] * 3,
        out_specs=whole(),
        cost_estimate=priced(12 * tile * (qx - 2) * (qy - 2)),
        compiler_params=granted(20),
        name="third",
    )(h2, e3, bias3)

    return pl.pallas_call(
        functools.partial(final_kernel, cells),
        out_shape=(
            jax.ShapeDtypeStruct(v.shape, f32),
            jax.ShapeDtypeStruct((6,) + v.shape[1:], f32),
        ),
        in_specs=[whole()] * 6,
        out_specs=(whole(), whole()),
        scratch_shapes=[pltpu.VMEM((2 * (qx - 3), 8 * 2 * (qy - 3), depth), f32)],
        cost_estimate=priced(8 * tile * (qx - 3) * (qy - 3)),
        compiler_params=granted(20),
        name="final",
    )(h3, e4, near, strip, far, energy)


def solution(mesh):
    block = P(None, axis_x, axis_y, None)
    return jax.shard_map(
        local,
        mesh=mesh,
        in_specs=(block,) + (P(),) * 7,
        out_specs=(block, block),
        check_vma=False,
    )
```

```python
import functools

import jax
import jax.numpy as jnp
from jax import lax
from jax.experimental import pallas as pl
from jax.experimental.pallas import tpu as pltpu
from jax.sharding import PartitionSpec as P

time_step = 0.1
viscosity = 0.05
power_input = 5.0
pairing = ((0, 3, 4), (3, 1, 5), (4, 5, 2))
halo = 6
axis_x = ("grp", "gx")
axis_y = "gy"
groups = 8
f32 = jnp.float32
bf16 = jnp.bfloat16


def shifted(cells, axis, step):
    count = lax.axis_size(axis)
    return lax.ppermute(cells, axis, [(i, (i + step) % count) for i in range(count)])


def blocks_in(extent, count):
    size = 1
    while count % (2 * size) == 0 and 2 * size * extent <= extent + 2 * halo:
        size *= 2
    return size


def expand_hidden(w_ref, out_ref):
    outs, channels = w_ref.shape[3], w_ref.shape[4]
    zero = jnp.zeros((outs, channels), f32)
    blank = jnp.zeros((channels, 2 * outs), bf16)
    for dz in range(3):
        for xin in range(4):
            tall = []
            for dy in range(3):
                rows = [
                    w_ref[xin - xo, dy, dz].astype(f32) if 0 <= xin - xo <= 2 else zero
                    for xo in range(2)
                ]
                tall.append(jnp.concatenate(rows, axis=0).T.astype(bf16))
            for yin in range(4):
                base = ((dz * 4 + yin) * 4 + xin) * channels
                for yo in range(2):
                    piece = tall[yin - yo] if 0 <= yin - yo <= 2 else blank
                    out_ref[base : base + channels, yo * 2 * outs : (yo + 1) * 2 * outs] = piece


def selector(yo):
    row = lax.broadcasted_iota(jnp.int32, (128, 128), 0)
    column = lax.broadcasted_iota(jnp.int32, (128, 128), 1)
    group, yin, part = row >> 4, (row >> 2) & 3, row & 3
    one, two = jnp.where(group >= 3, 1, 0), jnp.where(group >= 6, 1, 0)
    along = one + two
    dz = group - 3 * along
    spare = part == 3
    along = jnp.where(spare, 2, along)
    dz = jnp.where(spare, 2, dz)
    part = jnp.where(spare, group, part)
    wanted = (yin - yo) * 32 + (3 * part + along) * 3 + dz
    fits = (yin >= yo) & (yin - yo <= 2) & (part <= 2) & (column == wanted)
    return jnp.where(fits, 1.0, 0.0).astype(bf16)


def expand_first(w_ref, out_ref, flat):
    features, outs = w_ref.shape[2], w_ref.shape[4]
    flat[...] = jnp.zeros_like(flat)
    for dx in range(3):
        for dy in range(3):
            for channel in range(features):
                row = dy * 32 + channel * 3
                flat[dx, row : row + 3, :] = w_ref[dx, dy, channel].astype(f32)
    zero = jnp.zeros(flat.shape[1:], f32)
    for yo in range(2):
        pick = selector(yo)
        for xin in range(4):
            sides = [flat[xin - xo] if 0 <= xin - xo <= 2 else zero for xo in range(2)]
            both = jnp.concatenate(sides, axis=1).astype(bf16)
            block = jnp.dot(pick, both, preferred_element_type=f32)
            out_ref[xin * 128 : (xin + 1) * 128, yo * 2 * outs : (yo + 1) * 2 * outs] = (
                block.astype(bf16)
            )


def expand_last(w_ref, out_ref):
    outs, channels = w_ref.shape[3], w_ref.shape[4]
    zero = jnp.zeros((8, channels), f32)
    pad = jnp.zeros((8 - outs, channels), f32)
    taps = {}
    for dx in range(3):
        for dy in range(3):
            for dz in range(3):
                taps[dx, dy, dz] = jnp.concatenate([w_ref[dx, dy, dz].astype(f32), pad], axis=0)
    for yin in range(4):
        for pair in range(2):
            column = []
            for dz in range(3):
                for yo in range(2):
                    for xo in range(2):
                        halves = []
                        for xin in (2 * pair, 2 * pair + 1):
                            dx, dy = xin - xo, yin - yo
                            inside = 0 <= dx <= 2 and 0 <= dy <= 2
                            halves.append(taps[dx, dy, dz] if inside else zero)
                        column.append(jnp.concatenate(halves, axis=1))
            base = (yin * 2 + pair) * 2 * channels
            out_ref[:, base : base + 2 * channels] = jnp.concatenate(column, axis=0).astype(bf16)


def first_kernel(w1, b1, out_ref, bias, flat):
    bias[...] = jnp.concatenate([b1[...]] * 4, axis=1)
    expand_first(w1, out_ref, flat)


def later_kernel(w2, w3, w4, o2, o3, o4):
    expand_hidden(w2, o2)
    expand_hidden(w3, o3)
    expand_last(w4, o4)


def ends_kernel(width, v, head, tail):
    parts, extent_x, extent_y = v.shape[:3]
    for c in range(parts):
        for x in range(extent_x):
            at = (c * extent_x + x) * width
            head[at : at + width, :] = v[c, x, 0:width, :]
            tail[at : at + width, :] = v[c, x, extent_y - width : extent_y, :]


def strip_kernel(v, left, right, strip, *rest):
    parts, extent_x, extent_y = v.shape[:3]
    width = left.shape[0] // (parts * extent_x)
    tall = extent_y + 2 * width
    for c in range(parts):
        for x in range(extent_x):
            source, at = (c * extent_x + x) * width, (c * extent_x + x) * tall
            middle = at + width
            strip[at:middle, :] = left[source : source + width, :]
            strip[middle : middle + extent_y, :] = v[c, x]
            strip[middle + extent_y : at + tall, :] = right[source : source + width, :]
    if rest:
        low, high, hold = rest
        reach = low.shape[0] // (parts * tall)
        for target, first in ((low, extent_x - reach), (high, 0)):
            for c in range(parts):
                start = (c * extent_x + first) * tall
                hold[c * reach * tall : (c + 1) * reach * tall, :] = strip[
                    start : start + reach * tall, :
                ]
            target[...] = hold[...].astype(target.dtype)


def whole():
    return pl.BlockSpec(memory_space=pltpu.VMEM)


def granted(mib):
    return pltpu.CompilerParams(vmem_limit_bytes=mib * 2**20)


def priced(flops):
    return pl.CostEstimate(flops=int(flops), bytes_accessed=10**6, transcendentals=0)


def ends(v, width):
    shape = jax.ShapeDtypeStruct((v.shape[0] * v.shape[1] * width, v.shape[3]), f32)
    return pl.pallas_call(
        functools.partial(ends_kernel, width),
        out_shape=(shape, shape),
        in_specs=[whole()],
        out_specs=(whole(), whole()),
        compiler_params=granted(4),
        name="ends",
    )(v)


def strips(v, left, right, reach):
    parts, extent_x, extent_y, depth = v.shape
    tall = extent_y + 2 * halo
    outs = [jax.ShapeDtypeStruct((parts * extent_x * tall, depth), f32)]
    scratch = []
    if reach:
        outs += [jax.ShapeDtypeStruct((parts * reach * tall, depth), f32)] * 2
        scratch = [pltpu.VMEM((parts * reach * tall, depth), f32)]
    return pl.pallas_call(
        strip_kernel,
        out_shape=outs,
        in_specs=[whole()] * 3,
        out_specs=[whole()] * len(outs),
        scratch_shapes=scratch,
        compiler_params=granted(4),
        name="strips",
    )(v, left, right)


def prepare_first(w1, b1):
    outs = w1.shape[3]
    w1 = jnp.transpose(w1, (0, 1, 4, 2, 3))
    return pl.pallas_call(
        first_kernel,
        out_shape=(
            jax.ShapeDtypeStruct((512, 4 * outs), bf16),
            jax.ShapeDtypeStruct((1, 4 * outs), f32),
        ),
        in_specs=[whole()] * 2,
        out_specs=(whole(),) * 2,
        scratch_shapes=[pltpu.VMEM((3, 128, outs), f32)],
        cost_estimate=pl.CostEstimate(flops=4 * 10**9, bytes_accessed=10**7, transcendentals=0),
        compiler_params=granted(10),
        name="prepare_first",
    )(w1, b1.reshape(1, -1))


def prepare_later(w2, w3, w4):
    outs, channels = w2.shape[3], w2.shape[4]
    return pl.pallas_call(
        later_kernel,
        out_shape=(
            jax.ShapeDtypeStruct((48 * channels, 4 * outs), bf16),
            jax.ShapeDtypeStruct((48 * channels, 4 * outs), bf16),
            jax.ShapeDtypeStruct((96, 16 * channels), bf16),
        ),
        in_specs=[whole()] * 3,
        out_specs=(whole(),) * 3,
        cost_estimate=priced(10**9),
        compiler_params=granted(10),
        name="prepare_later",
    )(w2, w3, w4)


def lay_rows(target, at, piece, x, wide, tall):
    for c in range(3):
        start = (c * wide + x) * tall
        target[at, pl.ds(c, tall, stride=4), :] = piece[start : start + tall, :]
    target[at, pl.ds(3, tall, stride=4), :] = jnp.zeros((tall, piece.shape[1]), f32)


def features(rows, at, depth):
    total = rows.shape[1]
    center = rows[at + 1, 4 : total - 4, :]
    diffs = (
        (rows[at + 2, 4 : total - 4, :] - rows[at, 4 : total - 4, :]) * 0.5,
        (rows[at + 1, 8:total, :] - rows[at + 1, 0 : total - 8, :]) * 0.5,
        (pltpu.roll(center, depth - 1, 1) - pltpu.roll(center, 1, 1)) * 0.5,
    )
    parts = []
    for j in range(3):
        for amount in (1, 0, depth - 1):
            parts.append(pltpu.roll(diffs[j], amount, 1) if amount else diffs[j])
    spare = parts.pop()
    lane = lax.broadcasted_iota(jnp.int32, spare.shape, 0) & 3
    for c in range(3):
        parts[c] = jnp.where(lane == 3, pltpu.roll(spare, 3 - c, 0), parts[c])
    turned = []
    for half in range((total // 4 - 2) // 2 - 1):
        block = jnp.concatenate([part[8 * half : 8 * half + 16] for part in parts], axis=0)
        turned.append(block.astype(bf16).T)
    return turned


def merge(block):
    return block.reshape(block.shape[0] * block.shape[1], block.shape[2])


def layer(left, weight, bias, store, depth, variants):
    total = jnp.dot(left, weight[...], preferred_element_type=f32)
    value = jnp.tanh(total + bias)
    value = value.reshape(value.shape[0] // depth, depth, value.shape[1])
    width = value.shape[2] // 2
    for dz, amount in enumerate((1, 0, depth - 1)):
        if dz not in variants:
            continue
        moved = pltpu.roll(value, amount, 1) if amount else value
        moved = moved.astype(bf16)
        for yo in range(2):
            store(dz, yo, moved[:, :, yo * width : (yo + 1) * width])


every = (0, 1, 2)


def gather_hidden(source, xp, variants):
    rows = source.shape[-3] - 1
    parts = []
    for dz in variants:
        for yin in range(4):
            for pair in range(2):
                where = (xp + pair, yin % 2, slice(yin // 2, yin // 2 + rows))
                parts.append(merge(source[where if len(source.shape) == 5 else (dz, *where)]))
    return jnp.concatenate(parts, axis=1)


def store_hidden(target, xp):
    def store(dz, yo, block):
        target[(xp, yo) if len(target.shape) == 5 else (dz, xp, yo)] = block

    return store


def inner_kernel(low, near, own, far, w1, bias, h1, turned, rows):
    depth, tall = own.shape[1], rows.shape[1] // 4
    wide = own.shape[0] // (3 * tall)
    at = 0
    for piece in (near, own, far):
        for x in range(wide):
            lay_rows(rows, at, piece, x, wide, tall)
            at += 1

    def one(x, carry):
        for half, block in enumerate(features(rows, x, depth)):
            turned[x, half] = block
        return carry

    lax.fori_loop(0, turned.shape[0], one, 0, unroll=True)

    def step(q, carry):
        left = jnp.concatenate([merge(turned[2 * q + a]) for a in range(4)], axis=1)
        layer(left, w1, bias[...], store_hidden(h1, q + low), depth, every)
        return carry

    lax.fori_loop(0, turned.shape[0] // 2 - 1, step, 0, unroll=True)


def outer_kernel(box, *refs):
    low, near, own, far, high, turned, w1, bias, _, h1, energy, rows, edges, ends = refs
    depth, tall = own.shape[1], rows.shape[2] // 4
    wide = own.shape[0] // (3 * tall)
    reach = low.shape[0] // (3 * tall)
    ends[0] = low[...].astype(f32)
    ends[1] = high[...].astype(f32)
    columns = [(ends.at[0], x, reach) for x in range(reach)]
    for piece in (near, own, far):
        columns += [(piece, x, wide) for x in range(wide)]
    columns += [(ends.at[1], x, reach) for x in range(reach)]
    need = rows.shape[1]
    edge = need - 2
    for side, part in enumerate((columns[:need], columns[-need:])):
        for at, (piece, x, extent) in enumerate(part):
            lay_rows(rows.at[side], at, piece, x, extent, tall)
        for at in range(edge):
            for half, block in enumerate(features(rows.at[side], at, depth)):
                edges[side, at, half] = block
    inside = turned.shape[0]
    held = [edges.at[0, k] for k in range(edge)] + [turned.at[k] for k in range(inside)]
    held += [edges.at[1, k] for k in range(edge)]
    pairs = h1.shape[1]
    for k in range(edge // 2):
        for xp in (k, pairs - 1 - k):
            left = jnp.concatenate([merge(held[2 * xp + a][...]) for a in range(4)], axis=1)
            layer(left, w1, bias[...], store_hidden(h1, xp), depth, every)
    low_x, span_x, low_y, span_y = box
    total = None
    for piece, x, extent in columns[low_x : low_x + span_x]:
        for c in range(3):
            start = (c * extent + x) * tall + low_y
            part = piece[start : start + span_y, :]
            total = part * part if total is None else total + part * part
    energy[...] = jnp.broadcast_to(0.5 * jnp.sum(total, keepdims=True), energy.shape)


def second_kernel(h1, w2, bias, h2):
    depth = h1.shape[4]

    def step(xp, carry):
        layer(gather_hidden(h1, xp, every), w2, jnp.concatenate([bias[...]] * 4, axis=1), store_hidden(h2, xp), depth, every)
        return carry

    lax.fori_loop(0, h2.shape[1], step, 0, unroll=True)


def third_kernel(h2, w3, bias, h3):
    depth = h2.shape[4]

    def step(xp, carry):
        layer(gather_hidden(h2, xp, every), w3, jnp.concatenate([bias[...]] * 4, axis=1), store_hidden(h3, xp), depth, (1,))
        return carry

    lax.fori_loop(0, h3.shape[0], step, 0, unroll=True)


def final_kernel(cells, h3, w4, near, own, far, energy, updated_ref, stress_ref, tau):
    depth = own.shape[1]
    forcing = power_input / (2.0 * (energy[0, 0] / cells) + 1e-06)

    def final(xp, carry):
        sides = lax.dot_general(
            w4[...],
            gather_hidden(h3, xp, (1,)),
            (((1,), (1,)), ((), ())),
            preferred_element_type=f32,
        )
        for yp in range(sides.shape[1] // depth):
            part = sides[:, yp * depth : (yp + 1) * depth]
            total = pltpu.roll(part[0:32], 1, 1) + part[32:64] + pltpu.roll(part[64:96], depth - 1, 1)
            for yo in range(2):
                for xo in range(2):
                    cell = (2 * yo + xo) * 8
                    row = (2 * yp + yo) * 8
                    tau[2 * xp + xo, row : row + 8, :] = total[cell : cell + 8]
        return carry

    lax.fori_loop(0, h3.shape[0] - 1, final, 0, unroll=True)

    own_x, own_y = updated_ref.shape[1], updated_ref.shape[2]

    def stress_at(c, x, y):
        return tau[x, pl.ds(y * 8 + c, own_y, stride=8), :]

    def turn(a, amount):
        return pltpu.roll(a, amount % depth, 1)

    def vel(i, x, y):
        piece, at = own, x
        if x < 0:
            piece, at = near, x + own_x
        elif x >= own_x:
            piece, at = far, x - own_x
        start = (i * own_x + at) * (own_y + 2 * halo) + halo + y
        return piece[start : start + own_y, :]

    for x in range(own_x):
        for c in range(6):
            stress_ref[c, x] = stress_at(c, x + 1, 1)
        center = [vel(i, x, 0) for i in range(3)]
        for i in range(3):
            xm, xp, ym, yp = vel(i, x - 1, 0), vel(i, x + 1, 0), vel(i, x, -1), vel(i, x, 1)
            zm, zp = turn(center[i], 1), turn(center[i], -1)
            advect = (
                center[0] * ((xp - xm) * 0.5)
                + center[1] * ((yp - ym) * 0.5)
                + center[2] * ((zp - zm) * 0.5)
            )
            laplacian = xp + xm + yp + ym + zm + zp - 6.0 * center[i]
            px, py, pz = pairing[i]
            along_z = stress_at(pz, x + 1, 1)
            divergence = (
                (stress_at(px, x + 2, 1) - stress_at(px, x, 1)) * 0.5
                + (stress_at(py, x + 1, 2) - stress_at(py, x + 1, 0)) * 0.5
                + (turn(along_z, -1) - turn(along_z, 1)) * 0.5
            )
            tendency = viscosity * laplacian - advect - divergence + forcing * center[i]
            updated_ref[i, x] = center[i] + time_step * tendency


def box_total(box, size_x, size_y):
    count_x, count_y = lax.axis_size(axis_x), lax.axis_size(axis_y)
    left_x, left_y = count_x // size_x, count_y // size_y
    if (left_x & (left_x - 1)) or (left_y & (left_y - 1)):
        return lax.psum(box, axis_x + (axis_y,)) / (size_x * size_y)
    while size_x < count_x:
        box = box + shifted(box, axis_x, size_x)
        size_x *= 2
    while size_y < count_y:
        box = box + shifted(box, axis_y, size_y)
        size_y *= 2
    return box


def local(v, w1, b1, w2, b2, w3, b3, w4):
    parts, own_x, own_y, depth = v.shape
    count_x, count_y = lax.axis_size(axis_x), lax.axis_size(axis_y)
    width = 2 * w2.shape[3]
    bias2, bias3 = b2.reshape(1, -1), b3.reshape(1, -1)
    head, tail = ends(v, halo)
    left, right = shifted(tail, axis_y, 1), shifted(head, axis_y, -1)
    e1, bias1 = prepare_first(w1, b1)
    left, right, e1, bias1 = lax.optimization_barrier((left, right, e1, bias1))
    edge = halo - own_x
    strip, low, high = strips(v, left, right, edge)
    w2, w3, w4, strip = lax.optimization_barrier((w2, w3, w4, strip))
    e2, e3, e4 = prepare_later(w2, w3, w4)
    near, far = shifted(strip, axis_x, 1), shifted(strip, axis_x, -1)
    low, high = shifted(low, axis_x, 2), shifted(high, axis_x, -2)

    wide_x, wide_y = own_x + 2 * halo, own_y + 2 * halo
    qx, qy = (wide_x - 4) // 2, (wide_y - 4) // 2
    inside = wide_x - 2 - 2 * edge
    h1_shape = jax.ShapeDtypeStruct((3, qx, 2, qy, depth, width), bf16)
    h2_shape = jax.ShapeDtypeStruct((3, qx - 1, 2, qy - 1, depth, width), bf16)

    tile = 2 * depth * 256 * 256
    h1, turned = pl.pallas_call(
        functools.partial(inner_kernel, edge // 2),
        out_shape=(h1_shape, jax.ShapeDtypeStruct((inside, qy, depth, 128), bf16)),
        in_specs=[whole()] * 5,
        out_specs=(whole(), whole()),
        scratch_shapes=[pltpu.VMEM((inside + 2, 4 * wide_y, depth), f32)],
        cost_estimate=priced(4 * tile * qx * qy),
        compiler_params=granted(12),
        name="inner",
    )(near, strip, far, e1, bias1)

    size_x, size_y = blocks_in(own_x, count_x), blocks_in(own_y, count_y)
    box = (
        (wide_x - size_x * own_x) // 2,
        size_x * own_x,
        (wide_y - size_y * own_y) // 2,
        size_y * own_y,
    )
    h1, energy = pl.pallas_call(
        functools.partial(outer_kernel, box),
        out_shape=(h1_shape, jax.ShapeDtypeStruct((1, 1, 1, depth), f32)),
        in_specs=[whole()] * 9,
        out_specs=(whole(), whole()),
        scratch_shapes=[
            pltpu.VMEM((2, edge + 2, 4 * wide_y, depth), f32),
            pltpu.VMEM((2, edge, qy, depth, 128), bf16),
            pltpu.VMEM((2,) + low.shape, f32),
        ],
        input_output_aliases={8: 0},
        cost_estimate=priced(2 * tile * qx * qy),
        compiler_params=granted(12),
        name="outer",
    )(low, near, strip, far, high, turned, e1, bias1, h1)

    h2 = pl.pallas_call(
        second_kernel,
        out_shape=h2_shape,
        in_specs=[whole()] * 3,
        out_specs=whole(),
        cost_estimate=priced(12 * tile * (qx - 1) * (qy - 1)),
        compiler_params=granted(20),
        name="second",
    )(h1, e2, bias2)

    energy = box_total(energy, size_x, size_y)
    cells = own_x * own_y * depth * count_x * count_y

    h3 = pl.pallas_call(
        third_kernel,
        out_shape=jax.ShapeDtypeStruct((qx - 2, 2, qy - 2, depth, width), bf16),
        in_specs=[whole()] * 3,
        out_specs=whole(),
        cost_estimate=priced(12 * tile * (qx - 2) * (qy - 2)),
        compiler_params=granted(20),
        name="third",
    )(h2, e3, bias3)

    return pl.pallas_call(
        functools.partial(final_kernel, cells),
        out_shape=(
            jax.ShapeDtypeStruct(v.shape, f32),
            jax.ShapeDtypeStruct((6,) + v.shape[1:], f32),
        ),
        in_specs=[whole()] * 6,
        out_specs=(whole(), whole()),
        scratch_shapes=[pltpu.VMEM((2 * (qx - 3), 8 * 2 * (qy - 3), depth), f32)],
        cost_estimate=priced(8 * tile * (qx - 3) * (qy - 3)),
        compiler_params=granted(20),
        name="final",
    )(h3, e4, near, strip, far, energy)


def solution(mesh):
    block = P(None, axis_x, axis_y, None)
    return jax.shard_map(
        local,
        mesh=mesh,
        in_specs=(block,) + (P(),) * 7,
        out_specs=(block, block),
        check_vma=False,
    )
```

```python
import functools

import jax
import jax.numpy as jnp
from jax import lax
from jax.experimental import pallas as pl
from jax.experimental.pallas import tpu as pltpu
from jax.sharding import PartitionSpec as P

time_step = 0.1
viscosity = 0.05
power_input = 5.0
pairing = ((0, 3, 4), (3, 1, 5), (4, 5, 2))
halo = 6
axis_x = ("grp", "gx")
axis_y = "gy"
groups = 8
f32 = jnp.float32
bf16 = jnp.bfloat16


def shifted(cells, axis, step):
    count = lax.axis_size(axis)
    return lax.ppermute(cells, axis, [(i, (i + step) % count) for i in range(count)])


def swapped(cells, axis, odd):
    count = lax.axis_size(axis)
    order = [(i, (i + 1 if i % 2 == odd else i - 1) % count) for i in range(count)]
    return lax.ppermute(cells, axis, order)


def blocks_in(extent, count):
    size = 1
    while count % (2 * size) == 0 and 2 * size * extent <= extent + 2 * halo:
        size *= 2
    return size


def expand_hidden(w_ref, out_ref):
    outs, channels = w_ref.shape[3], w_ref.shape[4]
    zero = jnp.zeros((outs, channels), f32)
    blank = jnp.zeros((channels, 2 * outs), bf16)
    for dz in range(3):
        for xin in range(4):
            tall = []
            for dy in range(3):
                rows = [
                    w_ref[xin - xo, dy, dz].astype(f32) if 0 <= xin - xo <= 2 else zero
                    for xo in range(2)
                ]
                tall.append(jnp.concatenate(rows, axis=0).T.astype(bf16))
            for yin in range(4):
                base = ((dz * 4 + yin) * 4 + xin) * channels
                for yo in range(2):
                    piece = tall[yin - yo] if 0 <= yin - yo <= 2 else blank
                    out_ref[base : base + channels, yo * 2 * outs : (yo + 1) * 2 * outs] = piece


def selector(yo):
    row = lax.broadcasted_iota(jnp.int32, (128, 128), 0)
    column = lax.broadcasted_iota(jnp.int32, (128, 128), 1)
    group, yin, part = row >> 4, (row >> 2) & 3, row & 3
    one, two = jnp.where(group >= 3, 1, 0), jnp.where(group >= 6, 1, 0)
    along = one + two
    dz = group - 3 * along
    spare = part == 3
    along = jnp.where(spare, 2, along)
    dz = jnp.where(spare, 2, dz)
    part = jnp.where(spare, group, part)
    wanted = (yin - yo) * 32 + (3 * part + along) * 3 + dz
    fits = (yin >= yo) & (yin - yo <= 2) & (part <= 2) & (column == wanted)
    return jnp.where(fits, 1.0, 0.0).astype(bf16)


def expand_first(w_ref, out_ref, flat):
    features, outs = w_ref.shape[2], w_ref.shape[4]
    flat[...] = jnp.zeros_like(flat)
    for dx in range(3):
        for dy in range(3):
            for channel in range(features):
                row = dy * 32 + channel * 3
                flat[dx, row : row + 3, :] = w_ref[dx, dy, channel].astype(f32)
    zero = jnp.zeros(flat.shape[1:], f32)
    for yo in range(2):
        pick = selector(yo)
        for xin in range(4):
            sides = [flat[xin - xo] if 0 <= xin - xo <= 2 else zero for xo in range(2)]
            both = jnp.concatenate(sides, axis=1).astype(bf16)
            block = jnp.dot(pick, both, preferred_element_type=f32)
            out_ref[xin * 128 : (xin + 1) * 128, yo * 2 * outs : (yo + 1) * 2 * outs] = (
                block.astype(bf16)
            )


def expand_last(w_ref, out_ref):
    outs, channels = w_ref.shape[3], w_ref.shape[4]
    zero = jnp.zeros((8, channels), f32)
    pad = jnp.zeros((8 - outs, channels), f32)
    for pair in range(2):
        column = []
        for dy in range(3):
            for dz in range(3):
                for xo in range(2):
                    halves = []
                    for dx in (2 * pair - xo, 2 * pair + 1 - xo):
                        if 0 <= dx <= 2:
                            tap = w_ref[dx, dy, dz].astype(f32)
                            halves.append(jnp.concatenate([tap, pad], axis=0))
                        else:
                            halves.append(zero)
                    column.append(jnp.concatenate(halves, axis=1))
        base = pair * 2 * channels
        out_ref[:, base : base + 2 * channels] = jnp.concatenate(column, axis=0).astype(bf16)


def first_kernel(w1, b1, out_ref, bias, flat):
    bias[...] = jnp.concatenate([b1[...]] * 4, axis=1)
    expand_first(w1, out_ref, flat)


def later_kernel(w2, w3, w4, o2, o3, o4):
    expand_hidden(w2, o2)
    expand_hidden(w3, o3)
    expand_last(w4, o4)


def ends_kernel(width, v, head, tail):
    parts, extent_x, extent_y = v.shape[:3]
    for c in range(parts):
        for x in range(extent_x):
            at = (c * extent_x + x) * width
            head[at : at + width, :] = v[c, x, 0:width, :]
            tail[at : at + width, :] = v[c, x, extent_y - width : extent_y, :]


def strip_kernel(v, left, right, strip, *rest):
    parts, extent_x, extent_y = v.shape[:3]
    width = left.shape[0] // (parts * extent_x)
    tall = extent_y + 2 * width
    for c in range(parts):
        for x in range(extent_x):
            source, at = (c * extent_x + x) * width, (c * extent_x + x) * tall
            middle = at + width
            strip[at:middle, :] = left[source : source + width, :]
            strip[middle : middle + extent_y, :] = v[c, x]
            strip[middle + extent_y : at + tall, :] = right[source : source + width, :]
    if rest:
        low, high, hold = rest
        reach = low.shape[0] // (parts * tall)
        for target, first in ((low, extent_x - reach), (high, 0)):
            for c in range(parts):
                start = (c * extent_x + first) * tall
                hold[c * reach * tall : (c + 1) * reach * tall, :] = strip[
                    start : start + reach * tall, :
                ]
            target[...] = hold[...].astype(target.dtype)


def whole():
    return pl.BlockSpec(memory_space=pltpu.VMEM)


def granted(mib):
    return pltpu.CompilerParams(vmem_limit_bytes=mib * 2**20)


def priced(flops):
    return pl.CostEstimate(flops=int(flops), bytes_accessed=10**6, transcendentals=0)


def ends(v, width):
    shape = jax.ShapeDtypeStruct((v.shape[0] * v.shape[1] * width, v.shape[3]), f32)
    return pl.pallas_call(
        functools.partial(ends_kernel, width),
        out_shape=(shape, shape),
        in_specs=[whole()],
        out_specs=(whole(), whole()),
        compiler_params=granted(4),
        name="ends",
    )(v)


def strips(v, left, right, reach):
    parts, extent_x, extent_y, depth = v.shape
    tall = extent_y + 2 * halo
    outs = [jax.ShapeDtypeStruct((parts * extent_x * tall, depth), f32)]
    scratch = []
    if reach:
        outs += [jax.ShapeDtypeStruct((parts * reach * tall, depth), f32)] * 2
        scratch = [pltpu.VMEM((parts * reach * tall, depth), f32)]
    return pl.pallas_call(
        strip_kernel,
        out_shape=outs,
        in_specs=[whole()] * 3,
        out_specs=[whole()] * len(outs),
        scratch_shapes=scratch,
        compiler_params=granted(4),
        name="strips",
    )(v, left, right)


def prepare_first(w1, b1):
    outs = w1.shape[3]
    w1 = jnp.transpose(w1, (0, 1, 4, 2, 3))
    return pl.pallas_call(
        first_kernel,
        out_shape=(
            jax.ShapeDtypeStruct((512, 4 * outs), bf16),
            jax.ShapeDtypeStruct((1, 4 * outs), f32),
        ),
        in_specs=[whole()] * 2,
        out_specs=(whole(),) * 2,
        scratch_shapes=[pltpu.VMEM((3, 128, outs), f32)],
        cost_estimate=pl.CostEstimate(flops=4 * 10**9, bytes_accessed=10**7, transcendentals=0),
        compiler_params=granted(10),
        name="prepare_first",
    )(w1, b1.reshape(1, -1))


def prepare_later(w2, w3, w4):
    outs, channels = w2.shape[3], w2.shape[4]
    return pl.pallas_call(
        later_kernel,
        out_shape=(
            jax.ShapeDtypeStruct((48 * channels, 4 * outs), bf16),
            jax.ShapeDtypeStruct((48 * channels, 4 * outs), bf16),
            jax.ShapeDtypeStruct((144, 4 * channels), bf16),
        ),
        in_specs=[whole()] * 3,
        out_specs=(whole(),) * 3,
        cost_estimate=priced(10**9),
        compiler_params=granted(10),
        name="prepare_later",
    )(w2, w3, w4)


def lay_rows(target, at, piece, x, wide, tall):
    for c in range(3):
        start = (c * wide + x) * tall
        target[at, pl.ds(c, tall, stride=4), :] = piece[start : start + tall, :]
    target[at, pl.ds(3, tall, stride=4), :] = jnp.zeros((tall, piece.shape[1]), f32)


def features(rows, at, depth):
    total = rows.shape[1]
    center = rows[at + 1, 4 : total - 4, :]
    diffs = (
        (rows[at + 2, 4 : total - 4, :] - rows[at, 4 : total - 4, :]) * 0.5,
        (rows[at + 1, 8:total, :] - rows[at + 1, 0 : total - 8, :]) * 0.5,
        (pltpu.roll(center, depth - 1, 1) - pltpu.roll(center, 1, 1)) * 0.5,
    )
    parts = []
    for j in range(3):
        for amount in (1, 0, depth - 1):
            parts.append(pltpu.roll(diffs[j], amount, 1) if amount else diffs[j])
    spare = parts.pop()
    lane = lax.broadcasted_iota(jnp.int32, spare.shape, 0) & 3
    for c in range(3):
        parts[c] = jnp.where(lane == 3, pltpu.roll(spare, 3 - c, 0), parts[c])
    turned = []
    for half in range((total // 4 - 2) // 2 - 1):
        block = jnp.concatenate([part[8 * half : 8 * half + 16] for part in parts], axis=0)
        turned.append(block.astype(bf16).T)
    return turned


def merge(block):
    return block.reshape((block.shape[0] * block.shape[1],) + block.shape[2:])


def layer(left, weight, bias, store, depth, variants):
    total = jnp.dot(left, weight[...], preferred_element_type=f32)
    value = jnp.tanh(total + bias)
    value = value.reshape(value.shape[0] // depth, depth, value.shape[1])
    width = value.shape[2] // 2
    for dz, amount in enumerate((1, 0, depth - 1)):
        if dz not in variants:
            continue
        moved = pltpu.roll(value, amount, 1) if amount else value
        moved = moved.astype(bf16)
        for yo in range(2):
            store(dz, yo, moved[:, :, yo * width : (yo + 1) * width])


every = (0, 1, 2)


def gather_hidden(source, xp, variants):
    rows = source.shape[-3] - 1
    parts = []
    for dz in variants:
        for yin in range(4):
            for pair in range(2):
                where = (xp + pair, yin % 2, slice(yin // 2, yin // 2 + rows))
                parts.append(merge(source[where if len(source.shape) == 5 else (dz, *where)]))
    return jnp.concatenate(parts, axis=1)


def store_hidden(target, xp):
    def store(dz, yo, block):
        target[(xp, yo) if len(target.shape) == 5 else (dz, xp, yo)] = block

    return store


def inner_kernel(low, odd, apart, own, twin, w1, bias, h1, turned, sides, rows):
    depth, tall = own.shape[1], rows.shape[1] // 4
    wide = own.shape[0] // (3 * tall)
    right = odd[0]
    sides[right] = apart[...]
    sides[1 - right] = twin[...]
    for piece, at in ((apart, right * 2 * wide), (own, wide), (twin, (1 - right) * 2 * wide)):
        for x in range(wide):
            lay_rows(rows, at + x, piece, x, wide, tall)

    def one(x, carry):
        for half, block in enumerate(features(rows, x, depth)):
            turned[x, half] = block
        return carry

    lax.fori_loop(0, turned.shape[0], one, 0, unroll=True)

    def step(q, carry):
        left = jnp.concatenate([merge(turned[2 * q + a]) for a in range(4)], axis=1)
        layer(left, w1, bias[...], store_hidden(h1, q + low), depth, every)
        return carry

    lax.fori_loop(0, turned.shape[0] // 2 - 1, step, 0, unroll=True)


def outer_kernel(box, *refs):
    low, own, sides, high, turned, w1, bias, _, h1, energy, rows, edges, ends = refs
    near, far = sides.at[0], sides.at[1]
    depth, tall = own.shape[1], rows.shape[2] // 4
    wide = own.shape[0] // (3 * tall)
    reach = low.shape[0] // (3 * tall)
    ends[0] = low[...].astype(f32)
    ends[1] = high[...].astype(f32)
    columns = [(ends.at[0], x, reach) for x in range(reach)]
    for piece in (near, own, far):
        columns += [(piece, x, wide) for x in range(wide)]
    columns += [(ends.at[1], x, reach) for x in range(reach)]
    need = rows.shape[1]
    edge = need - 2
    for side, part in enumerate((columns[:need], columns[-need:])):
        for at, (piece, x, extent) in enumerate(part):
            lay_rows(rows.at[side], at, piece, x, extent, tall)
        for at in range(edge):
            for half, block in enumerate(features(rows.at[side], at, depth)):
                edges[side, at, half] = block
    inside = turned.shape[0]
    held = [edges.at[0, k] for k in range(edge)] + [turned.at[k] for k in range(inside)]
    held += [edges.at[1, k] for k in range(edge)]
    pairs = h1.shape[1]
    for k in range(edge // 2):
        for xp in (k, pairs - 1 - k):
            left = jnp.concatenate([merge(held[2 * xp + a][...]) for a in range(4)], axis=1)
            layer(left, w1, bias[...], store_hidden(h1, xp), depth, every)
    low_x, span_x, low_y, span_y = box
    total = None
    for piece, x, extent in columns[low_x : low_x + span_x]:
        for c in range(3):
            start = (c * extent + x) * tall + low_y
            part = piece[start : start + span_y, :]
            total = part * part if total is None else total + part * part
    energy[...] = jnp.broadcast_to(0.5 * jnp.sum(total, keepdims=True), energy.shape)


def second_kernel(h1, w2, bias, h2):
    depth = h1.shape[4]

    def step(xp, carry):
        layer(gather_hidden(h1, xp, every), w2, jnp.concatenate([bias[...]] * 4, axis=1), store_hidden(h2, xp), depth, every)
        return carry

    lax.fori_loop(0, h2.shape[1], step, 0, unroll=True)


def third_kernel(h2, w3, bias, h3):
    depth = h2.shape[4]

    def step(xp, carry):
        layer(gather_hidden(h2, xp, every), w3, jnp.concatenate([bias[...]] * 4, axis=1), store_hidden(h3, xp), depth, (1,))
        return carry

    lax.fori_loop(0, h3.shape[0], step, 0, unroll=True)


def final_kernel(cells, h3, w4, own, sides, energy, updated_ref, stress_ref, tau):
    near, far = sides.at[0], sides.at[1]
    depth = own.shape[1]
    forcing = power_input / (2.0 * (energy[0, 0] / cells) + 1e-06)

    rows = h3.shape[2]

    def final(xp, carry):
        cells = [merge(merge(h3[xp + pair])) for pair in range(2)]
        sides = lax.dot_general(
            w4[...],
            jnp.concatenate(cells, axis=1),
            (((1,), (1,)), ((), ())),
            preferred_element_type=f32,
        )
        for y in range(2 * rows - 2):
            sums = []
            for dz in range(3):
                total = None
                for dy in range(3):
                    at = ((y + dy) % 2 * rows + (y + dy) // 2) * depth
                    tap = (3 * dy + dz) * 16
                    part = sides[tap : tap + 16, at : at + depth]
                    total = part if total is None else total + part
                sums.append(total)
            total = pltpu.roll(sums[0], 1, 1) + sums[1] + pltpu.roll(sums[2], depth - 1, 1)
            for xo in range(2):
                tau[2 * xp + xo, y * 8 : y * 8 + 8, :] = total[xo * 8 : xo * 8 + 8]
        return carry

    lax.fori_loop(0, h3.shape[0] - 1, final, 0, unroll=True)

    own_x, own_y = updated_ref.shape[1], updated_ref.shape[2]

    def stress_at(c, x, y):
        return tau[x, pl.ds(y * 8 + c, own_y, stride=8), :]

    def turn(a, amount):
        return pltpu.roll(a, amount % depth, 1)

    def vel(i, x, y):
        piece, at = own, x
        if x < 0:
            piece, at = near, x + own_x
        elif x >= own_x:
            piece, at = far, x - own_x
        start = (i * own_x + at) * (own_y + 2 * halo) + halo + y
        return piece[start : start + own_y, :]

    for x in range(own_x):
        for c in range(6):
            stress_ref[c, x] = stress_at(c, x + 1, 1)
        center = [vel(i, x, 0) for i in range(3)]
        for i in range(3):
            xm, xp, ym, yp = vel(i, x - 1, 0), vel(i, x + 1, 0), vel(i, x, -1), vel(i, x, 1)
            zm, zp = turn(center[i], 1), turn(center[i], -1)
            advect = (
                center[0] * ((xp - xm) * 0.5)
                + center[1] * ((yp - ym) * 0.5)
                + center[2] * ((zp - zm) * 0.5)
            )
            laplacian = xp + xm + yp + ym + zm + zp - 6.0 * center[i]
            px, py, pz = pairing[i]
            along_z = stress_at(pz, x + 1, 1)
            divergence = (
                (stress_at(px, x + 2, 1) - stress_at(px, x, 1)) * 0.5
                + (stress_at(py, x + 1, 2) - stress_at(py, x + 1, 0)) * 0.5
                + (turn(along_z, -1) - turn(along_z, 1)) * 0.5
            )
            tendency = viscosity * laplacian - advect - divergence + forcing * center[i]
            updated_ref[i, x] = center[i] + time_step * tendency


def box_total(box, size_x, size_y):
    count_x, count_y = lax.axis_size(axis_x), lax.axis_size(axis_y)
    left_x, left_y = count_x // size_x, count_y // size_y
    if (left_x & (left_x - 1)) or (left_y & (left_y - 1)):
        return lax.psum(box, axis_x + (axis_y,)) / (size_x * size_y)
    while size_x < count_x:
        box = box + shifted(box, axis_x, size_x)
        size_x *= 2
    while size_y < count_y:
        box = box + shifted(box, axis_y, size_y)
        size_y *= 2
    return box


def local(v, w1, b1, w2, b2, w3, b3, w4):
    parts, own_x, own_y, depth = v.shape
    count_x, count_y = lax.axis_size(axis_x), lax.axis_size(axis_y)
    width = 2 * w2.shape[3]
    bias2, bias3 = b2.reshape(1, -1), b3.reshape(1, -1)
    head, tail = ends(v, halo)
    left, right = shifted(tail, axis_y, 1), shifted(head, axis_y, -1)
    e1, bias1 = prepare_first(w1, b1)
    left, right, e1, bias1 = lax.optimization_barrier((left, right, e1, bias1))
    edge = halo - own_x
    strip, low, high = strips(v, left, right, edge)
    w2, w3, w4, strip = lax.optimization_barrier((w2, w3, w4, strip))
    e2, e3, e4 = prepare_later(w2, w3, w4)
    apart, twin = swapped(strip, axis_x, 1), swapped(strip, axis_x, 0)
    odd = (lax.axis_index(axis_x) % 2).reshape(1)
    low, high = shifted(low, axis_x, 2), shifted(high, axis_x, -2)

    wide_x, wide_y = own_x + 2 * halo, own_y + 2 * halo
    qx, qy = (wide_x - 4) // 2, (wide_y - 4) // 2
    inside = wide_x - 2 - 2 * edge
    h1_shape = jax.ShapeDtypeStruct((3, qx, 2, qy, depth, width), bf16)
    h2_shape = jax.ShapeDtypeStruct((3, qx - 1, 2, qy - 1, depth, width), bf16)

    tile = 2 * depth * 256 * 256
    h1, turned, sides = pl.pallas_call(
        functools.partial(inner_kernel, edge // 2),
        out_shape=(
            h1_shape,
            jax.ShapeDtypeStruct((inside, qy, depth, 128), bf16),
            jax.ShapeDtypeStruct((2,) + strip.shape, f32),
        ),
        in_specs=[pl.BlockSpec(memory_space=pltpu.SMEM)] + [whole()] * 5,
        out_specs=(whole(),) * 3,
        scratch_shapes=[pltpu.VMEM((inside + 2, 4 * wide_y, depth), f32)],
        cost_estimate=priced(4 * tile * qx * qy),
        compiler_params=granted(12),
        name="inner",
    )(odd, apart, strip, twin, e1, bias1)

    size_x, size_y = blocks_in(own_x, count_x), blocks_in(own_y, count_y)
    box = (
        (wide_x - size_x * own_x) // 2,
        size_x * own_x,
        (wide_y - size_y * own_y) // 2,
        size_y * own_y,
    )
    h1, energy = pl.pallas_call(
        functools.partial(outer_kernel, box),
        out_shape=(h1_shape, jax.ShapeDtypeStruct((1, 1, 1, depth), f32)),
        in_specs=[whole()] * 8,
        out_specs=(whole(), whole()),
        scratch_shapes=[
            pltpu.VMEM((2, edge + 2, 4 * wide_y, depth), f32),
            pltpu.VMEM((2, edge, qy, depth, 128), bf16),
            pltpu.VMEM((2,) + low.shape, f32),
        ],
        input_output_aliases={7: 0},
        cost_estimate=priced(2 * tile * qx * qy),
        compiler_params=granted(12),
        name="outer",
    )(low, strip, sides, high, turned, e1, bias1, h1)

    h2 = pl.pallas_call(
        second_kernel,
        out_shape=h2_shape,
        in_specs=[whole()] * 3,
        out_specs=whole(),
        cost_estimate=priced(12 * tile * (qx - 1) * (qy - 1)),
        compiler_params=granted(20),
        name="second",
    )(h1, e2, bias2)

    energy = box_total(energy, size_x, size_y)
    cells = own_x * own_y * depth * count_x * count_y

    h3 = pl.pallas_call(
        third_kernel,
        out_shape=jax.ShapeDtypeStruct((qx - 2, 2, qy - 2, depth, width), bf16),
        in_specs=[whole()] * 3,
        out_specs=whole(),
        cost_estimate=priced(12 * tile * (qx - 2) * (qy - 2)),
        compiler_params=granted(20),
        name="third",
    )(h2, e3, bias3)

    return pl.pallas_call(
        functools.partial(final_kernel, cells),
        out_shape=(
            jax.ShapeDtypeStruct(v.shape, f32),
            jax.ShapeDtypeStruct((6,) + v.shape[1:], f32),
        ),
        in_specs=[whole()] * 5,
        out_specs=(whole(), whole()),
        scratch_shapes=[pltpu.VMEM((2 * (qx - 3), 8 * 2 * (qy - 3), depth), f32)],
        cost_estimate=priced(8 * tile * (qx - 3) * (qy - 3)),
        compiler_params=granted(20),
        name="final",
    )(h3, e4, strip, sides, energy)


def solution(mesh):
    block = P(None, axis_x, axis_y, None)
    return jax.shard_map(
        local,
        mesh=mesh,
        in_specs=(block,) + (P(),) * 7,
        out_specs=(block, block),
        check_vma=False,
    )
```

```python
import functools

import jax
import jax.numpy as jnp
from jax import lax
from jax.experimental import pallas as pl
from jax.experimental.pallas import tpu as pltpu
from jax.sharding import PartitionSpec as P

time_step = 0.1
viscosity = 0.05
power_input = 5.0
pairing = ((0, 3, 4), (3, 1, 5), (4, 5, 2))
halo = 6
axis_x = ("grp", "gx")
axis_y = "gy"
groups = 8
f32 = jnp.float32
bf16 = jnp.bfloat16


def shifted(cells, axis, step):
    count = lax.axis_size(axis)
    return lax.ppermute(cells, axis, [(i, (i + step) % count) for i in range(count)])


def swapped(cells, axis, odd):
    count = lax.axis_size(axis)
    order = [(i, (i + 1 if i % 2 == odd else i - 1) % count) for i in range(count)]
    return lax.ppermute(cells, axis, order)


def crossed(cells, axis):
    count = lax.axis_size(axis)
    return lax.ppermute(cells, axis, [(i, (i - 2 if i % 2 else i + 2) % count) for i in range(count)])


def blocks_in(extent, count):
    size = 1
    while count % (2 * size) == 0 and 2 * size * extent <= extent + 2 * halo:
        size *= 2
    return size


def expand_hidden(w_ref, out_ref):
    outs, channels = w_ref.shape[3], w_ref.shape[4]
    zero = jnp.zeros((outs, channels), f32)
    blank = jnp.zeros((channels, 2 * outs), bf16)
    for dz in range(3):
        for xin in range(4):
            tall = []
            for dy in range(3):
                rows = [
                    w_ref[xin - xo, dy, dz].astype(f32) if 0 <= xin - xo <= 2 else zero
                    for xo in range(2)
                ]
                tall.append(jnp.concatenate(rows, axis=0).T.astype(bf16))
            for yin in range(4):
                base = ((dz * 4 + yin) * 4 + xin) * channels
                for yo in range(2):
                    piece = tall[yin - yo] if 0 <= yin - yo <= 2 else blank
                    out_ref[base : base + channels, yo * 2 * outs : (yo + 1) * 2 * outs] = piece


def selector(yo):
    row = lax.broadcasted_iota(jnp.int32, (128, 128), 0)
    column = lax.broadcasted_iota(jnp.int32, (128, 128), 1)
    group, yin, part = row >> 4, (row >> 2) & 3, row & 3
    one, two = jnp.where(group >= 3, 1, 0), jnp.where(group >= 6, 1, 0)
    along = one + two
    dz = group - 3 * along
    spare = part == 3
    along = jnp.where(spare, 2, along)
    dz = jnp.where(spare, 2, dz)
    part = jnp.where(spare, group, part)
    wanted = (yin - yo) * 32 + (3 * part + along) * 3 + dz
    fits = (yin >= yo) & (yin - yo <= 2) & (part <= 2) & (column == wanted)
    return jnp.where(fits, 1.0, 0.0).astype(bf16)


def expand_first(w_ref, out_ref, flat):
    features, outs = w_ref.shape[2], w_ref.shape[4]
    flat[...] = jnp.zeros_like(flat)
    for dx in range(3):
        for dy in range(3):
            for channel in range(features):
                row = dy * 32 + channel * 3
                flat[dx, row : row + 3, :] = w_ref[dx, dy, channel].astype(f32)
    zero = jnp.zeros(flat.shape[1:], f32)
    for yo in range(2):
        pick = selector(yo)
        for xin in range(4):
            sides = [flat[xin - xo] if 0 <= xin - xo <= 2 else zero for xo in range(2)]
            both = jnp.concatenate(sides, axis=1).astype(bf16)
            block = jnp.dot(pick, both, preferred_element_type=f32)
            out_ref[xin * 128 : (xin + 1) * 128, yo * 2 * outs : (yo + 1) * 2 * outs] = (
                block.astype(bf16)
            )


def expand_last(w_ref, out_ref):
    outs, channels = w_ref.shape[3], w_ref.shape[4]
    zero = jnp.zeros((8, channels), f32)
    pad = jnp.zeros((8 - outs, channels), f32)
    for pair in range(2):
        column = []
        for dy in range(3):
            for dz in range(3):
                for xo in range(2):
                    halves = []
                    for dx in (2 * pair - xo, 2 * pair + 1 - xo):
                        if 0 <= dx <= 2:
                            tap = w_ref[dx, dy, dz].astype(f32)
                            halves.append(jnp.concatenate([tap, pad], axis=0))
                        else:
                            halves.append(zero)
                    column.append(jnp.concatenate(halves, axis=1))
        base = pair * 2 * channels
        out_ref[:, base : base + 2 * channels] = jnp.concatenate(column, axis=0).astype(bf16)


def first_kernel(w1, b1, out_ref, bias, flat):
    bias[...] = jnp.concatenate([b1[...]] * 4, axis=1)
    expand_first(w1, out_ref, flat)


def later_kernel(w2, w3, w4, o2, o3, o4):
    expand_hidden(w2, o2)
    expand_hidden(w3, o3)
    expand_last(w4, o4)


def ends_kernel(width, v, head, tail):
    parts, extent_x, extent_y = v.shape[:3]
    for c in range(parts):
        for x in range(extent_x):
            at = (c * extent_x + x) * width
            head[at : at + width, :] = v[c, x, 0:width, :]
            tail[at : at + width, :] = v[c, x, extent_y - width : extent_y, :]


def strip_kernel(odd, v, left, right, strip, piece):
    parts, extent_x, extent_y = v.shape[:3]
    width = left.shape[0] // (parts * extent_x)
    tall = extent_y + 2 * width
    for c in range(parts):
        for x in range(extent_x):
            source, at = (c * extent_x + x) * width, (c * extent_x + x) * tall
            middle = at + width
            strip[at:middle, :] = left[source : source + width, :]
            strip[middle : middle + extent_y, :] = v[c, x]
            strip[middle + extent_y : at + tall, :] = right[source : source + width, :]
    reach = piece.shape[0] // (parts * tall)
    size = reach * tall
    for c in range(parts):
        head = c * extent_x * tall
        tail = head + (extent_x - reach) * tall
        piece[c * size : (c + 1) * size, :] = jnp.where(
            odd[0] == 1, strip[head : head + size, :], strip[tail : tail + size, :]
        )


def energy_kernel(box, own, twin, energy):
    wide, tall, low, span = box
    total = None
    for piece in (own, twin):
        for k in range(3 * wide):
            part = piece[k * tall + low : k * tall + low + span, :]
            total = part * part if total is None else total + part * part
    energy[...] = jnp.broadcast_to(0.5 * jnp.sum(total, keepdims=True), energy.shape)


def whole():
    return pl.BlockSpec(memory_space=pltpu.VMEM)


def granted(mib):
    return pltpu.CompilerParams(vmem_limit_bytes=mib * 2**20)


def priced(flops):
    return pl.CostEstimate(flops=int(flops), bytes_accessed=10**6, transcendentals=0)


def ends(v, width):
    shape = jax.ShapeDtypeStruct((v.shape[0] * v.shape[1] * width, v.shape[3]), f32)
    return pl.pallas_call(
        functools.partial(ends_kernel, width),
        out_shape=(shape, shape),
        in_specs=[whole()],
        out_specs=(whole(), whole()),
        compiler_params=granted(4),
        name="ends",
    )(v)


def scalar():
    return pl.BlockSpec(memory_space=pltpu.SMEM)


def strips(odd, v, left, right, reach):
    parts, extent_x, extent_y, depth = v.shape
    tall = extent_y + 2 * halo
    return pl.pallas_call(
        strip_kernel,
        out_shape=(
            jax.ShapeDtypeStruct((parts * extent_x * tall, depth), f32),
            jax.ShapeDtypeStruct((parts * reach * tall, depth), f32),
        ),
        in_specs=[scalar()] + [whole()] * 3,
        out_specs=(whole(), whole()),
        compiler_params=granted(4),
        name="strips",
    )(odd, v, left, right)


def prepare_first(w1, b1):
    outs = w1.shape[3]
    w1 = jnp.transpose(w1, (0, 1, 4, 2, 3))
    return pl.pallas_call(
        first_kernel,
        out_shape=(
            jax.ShapeDtypeStruct((512, 4 * outs), bf16),
            jax.ShapeDtypeStruct((1, 4 * outs), f32),
        ),
        in_specs=[whole()] * 2,
        out_specs=(whole(),) * 2,
        scratch_shapes=[pltpu.VMEM((3, 128, outs), f32)],
        cost_estimate=pl.CostEstimate(flops=4 * 10**9, bytes_accessed=10**7, transcendentals=0),
        compiler_params=granted(10),
        name="prepare_first",
    )(w1, b1.reshape(1, -1))


def prepare_later(w2, w3, w4):
    outs, channels = w2.shape[3], w2.shape[4]
    return pl.pallas_call(
        later_kernel,
        out_shape=(
            jax.ShapeDtypeStruct((48 * channels, 4 * outs), bf16),
            jax.ShapeDtypeStruct((48 * channels, 4 * outs), bf16),
            jax.ShapeDtypeStruct((144, 4 * channels), bf16),
        ),
        in_specs=[whole()] * 3,
        out_specs=(whole(),) * 3,
        cost_estimate=priced(10**9),
        compiler_params=granted(10),
        name="prepare_later",
    )(w2, w3, w4)


def lay_rows(target, at, piece, x, wide, tall):
    for c in range(3):
        start = (c * wide + x) * tall
        target[at, pl.ds(c, tall, stride=4), :] = piece[start : start + tall, :]
    target[at, pl.ds(3, tall, stride=4), :] = jnp.zeros((tall, piece.shape[1]), f32)


def features(rows, at, depth):
    total = rows.shape[1]
    center = rows[at + 1, 4 : total - 4, :]
    diffs = (
        (rows[at + 2, 4 : total - 4, :] - rows[at, 4 : total - 4, :]) * 0.5,
        (rows[at + 1, 8:total, :] - rows[at + 1, 0 : total - 8, :]) * 0.5,
        (pltpu.roll(center, depth - 1, 1) - pltpu.roll(center, 1, 1)) * 0.5,
    )
    parts = []
    for j in range(3):
        for amount in (1, 0, depth - 1):
            parts.append(pltpu.roll(diffs[j], amount, 1) if amount else diffs[j])
    spare = parts.pop()
    lane = lax.broadcasted_iota(jnp.int32, spare.shape, 0) & 3
    for c in range(3):
        parts[c] = jnp.where(lane == 3, pltpu.roll(spare, 3 - c, 0), parts[c])
    turned = []
    for half in range((total // 4 - 2) // 2 - 1):
        block = jnp.concatenate([part[8 * half : 8 * half + 16] for part in parts], axis=0)
        turned.append(block.astype(bf16).T)
    return turned


def merge(block):
    return block.reshape((block.shape[0] * block.shape[1],) + block.shape[2:])


def layer(left, weight, bias, store, depth, variants):
    total = jnp.dot(left, weight[...], preferred_element_type=f32)
    value = jnp.tanh(total + bias)
    value = value.reshape(value.shape[0] // depth, depth, value.shape[1])
    width = value.shape[2] // 2
    for dz, amount in enumerate((1, 0, depth - 1)):
        if dz not in variants:
            continue
        moved = pltpu.roll(value, amount, 1) if amount else value
        moved = moved.astype(bf16)
        for yo in range(2):
            store(dz, yo, moved[:, :, yo * width : (yo + 1) * width])


every = (0, 1, 2)


def gather_hidden(source, xp, variants):
    rows = source.shape[-3] - 1
    parts = []
    for dz in variants:
        for yin in range(4):
            for pair in range(2):
                where = (xp + pair, yin % 2, slice(yin // 2, yin // 2 + rows))
                parts.append(merge(source[where if len(source.shape) == 5 else (dz, *where)]))
    return jnp.concatenate(parts, axis=1)


def store_hidden(target, xp):
    def store(dz, yo, block):
        target[(xp, yo) if len(target.shape) == 5 else (dz, xp, yo)] = block

    return store


def inner_kernel(edge, odd, apart, own, twin, w1, bias, h1, turned, sides, rows):
    depth, tall = own.shape[1], rows.shape[1] // 4
    wide = own.shape[0] // (3 * tall)
    right = odd[0]
    sides[right] = apart[...]
    sides[1 - right] = twin[...]
    for piece, at in ((apart, right * 2 * wide), (own, wide), (twin, (1 - right) * 2 * wide)):
        for x in range(wide):
            lay_rows(rows, at + x, piece, x, wide, tall)
    first = (1 - right) * edge
    inside = turned.shape[0] - edge

    def one(x, carry):
        for half, block in enumerate(features(rows, x, depth)):
            turned[x + first, half] = block
        return carry

    lax.fori_loop(0, inside, one, 0, unroll=True)
    low = (1 - right) * (edge // 2)

    def step(q, carry):
        left = jnp.concatenate([merge(turned[2 * q + first + a]) for a in range(4)], axis=1)
        layer(left, w1, bias[...], store_hidden(h1, q + low), depth, every)
        return carry

    lax.fori_loop(0, inside // 2 - 1, step, 0, unroll=True)


def outer_kernel(edge, odd, piece, sides, w1, bias, _, __, turned, h1, rows):
    depth, tall = piece.shape[1], rows.shape[1] // 4
    reach = piece.shape[0] // (3 * tall)
    wide = sides.shape[1] // (3 * tall)
    right = odd[0]
    for x in range(reach):
        lay_rows(rows, right * 2 + x, piece, x, reach, tall)
    near = sides.at[right]
    for x in range(2):
        for c in range(3):
            head = (c * wide + x) * tall
            tail = (c * wide + wide - 2 + x) * tall
            value = jnp.where(right == 1, near[tail : tail + tall, :], near[head : head + tall, :])
            rows[(1 - right) * reach + x, pl.ds(c, tall, stride=4), :] = value
        rows[(1 - right) * reach + x, pl.ds(3, tall, stride=4), :] = jnp.zeros((tall, depth), f32)
    base = right * (turned.shape[0] - edge)
    for at in range(edge):
        for half, block in enumerate(features(rows, at, depth)):
            turned[base + at, half] = block
    start = right * (turned.shape[0] - 2 - edge)
    for k in range(edge // 2):
        left = jnp.concatenate([merge(turned[start + 2 * k + a]) for a in range(4)], axis=1)
        xp = right * (h1.shape[1] - edge // 2) + k
        layer(left, w1, bias[...], store_hidden(h1, xp), depth, every)


def second_kernel(odd, h1, w2, bias, h2, gift):
    depth = h1.shape[4]

    def step(xp, carry):
        store = store_hidden(h2, xp + odd[0])
        layer(gather_hidden(h1, xp, every), w2, jnp.concatenate([bias[...]] * 4, axis=1), store, depth, every)
        return carry

    lax.fori_loop(0, h2.shape[1] - 1, step, 0, unroll=True)
    gift[...] = h2[:, h2.shape[1] // 2]


def alone_kernel(odd, h2, w3, bias, h3):
    depth = h2.shape[4]

    def step(k, carry):
        xp = k + odd[0]
        store = store_hidden(h3, xp)
        layer(gather_hidden(h2, xp, every), w3, jnp.concatenate([bias[...]] * 4, axis=1), store, depth, (1,))
        return carry

    lax.fori_loop(0, h3.shape[0] - 1, step, 0, unroll=True)


def shared_kernel(odd, gift, w3, bias, _, __, h2, h3):
    depth = h2.shape[4]
    h2[:, (1 - odd[0]) * (h2.shape[1] - 1)] = gift[...]
    xp = (1 - odd[0]) * (h3.shape[0] - 1)
    store = store_hidden(h3, xp)
    layer(gather_hidden(h2, xp, every), w3, jnp.concatenate([bias[...]] * 4, axis=1), store, depth, (1,))


def final_kernel(cells, h3, w4, own, sides, energy, updated_ref, stress_ref, tau):
    near, far = sides.at[0], sides.at[1]
    depth = own.shape[1]
    forcing = power_input / (2.0 * (energy[0, 0] / cells) + 1e-06)

    rows = h3.shape[2]

    def final(xp, carry):
        cells = [merge(merge(h3[xp + pair])) for pair in range(2)]
        sides = lax.dot_general(
            w4[...],
            jnp.concatenate(cells, axis=1),
            (((1,), (1,)), ((), ())),
            preferred_element_type=f32,
        )
        for y in range(2 * rows - 2):
            sums = []
            for dz in range(3):
                total = None
                for dy in range(3):
                    at = ((y + dy) % 2 * rows + (y + dy) // 2) * depth
                    tap = (3 * dy + dz) * 16
                    part = sides[tap : tap + 16, at : at + depth]
                    total = part if total is None else total + part
                sums.append(total)
            total = pltpu.roll(sums[0], 1, 1) + sums[1] + pltpu.roll(sums[2], depth - 1, 1)
            for xo in range(2):
                tau[2 * xp + xo, y * 8 : y * 8 + 8, :] = total[xo * 8 : xo * 8 + 8]
        return carry

    lax.fori_loop(0, h3.shape[0] - 1, final, 0, unroll=True)

    own_x, own_y = updated_ref.shape[1], updated_ref.shape[2]

    def stress_at(c, x, y):
        return tau[x, pl.ds(y * 8 + c, own_y, stride=8), :]

    def turn(a, amount):
        return pltpu.roll(a, amount % depth, 1)

    def vel(i, x, y):
        piece, at = own, x
        if x < 0:
            piece, at = near, x + own_x
        elif x >= own_x:
            piece, at = far, x - own_x
        start = (i * own_x + at) * (own_y + 2 * halo) + halo + y
        return piece[start : start + own_y, :]

    for x in range(own_x):
        for c in range(6):
            stress_ref[c, x] = stress_at(c, x + 1, 1)
        center = [vel(i, x, 0) for i in range(3)]
        for i in range(3):
            xm, xp, ym, yp = vel(i, x - 1, 0), vel(i, x + 1, 0), vel(i, x, -1), vel(i, x, 1)
            zm, zp = turn(center[i], 1), turn(center[i], -1)
            advect = (
                center[0] * ((xp - xm) * 0.5)
                + center[1] * ((yp - ym) * 0.5)
                + center[2] * ((zp - zm) * 0.5)
            )
            laplacian = xp + xm + yp + ym + zm + zp - 6.0 * center[i]
            px, py, pz = pairing[i]
            along_z = stress_at(pz, x + 1, 1)
            divergence = (
                (stress_at(px, x + 2, 1) - stress_at(px, x, 1)) * 0.5
                + (stress_at(py, x + 1, 2) - stress_at(py, x + 1, 0)) * 0.5
                + (turn(along_z, -1) - turn(along_z, 1)) * 0.5
            )
            tendency = viscosity * laplacian - advect - divergence + forcing * center[i]
            updated_ref[i, x] = center[i] + time_step * tendency


def box_rounds(size_x, size_y):
    count_x, count_y = lax.axis_size(axis_x), lax.axis_size(axis_y)
    rounds = []
    while size_x < count_x:
        rounds.append((axis_x, size_x))
        size_x *= 2
    while size_y < count_y:
        rounds.append((axis_y, size_y))
        size_y *= 2
    return rounds


def local(v, w1, b1, w2, b2, w3, b3, w4):
    parts, own_x, own_y, depth = v.shape
    count_x, count_y = lax.axis_size(axis_x), lax.axis_size(axis_y)
    width = 2 * w2.shape[3]
    bias2, bias3 = b2.reshape(1, -1), b3.reshape(1, -1)
    odd = (lax.axis_index(axis_x) % 2).reshape(1)
    head, tail = ends(v, halo)
    left, right = shifted(tail, axis_y, 1), shifted(head, axis_y, -1)
    e1, bias1 = prepare_first(w1, b1)
    left, right, e1, bias1 = lax.optimization_barrier((left, right, e1, bias1))
    edge = halo - own_x
    strip, piece = strips(odd, v, left, right, edge)
    w2, w3, w4, strip = lax.optimization_barrier((w2, w3, w4, strip))
    e2, e3, e4 = prepare_later(w2, w3, w4)
    apart, twin = swapped(strip, axis_x, 1), swapped(strip, axis_x, 0)
    piece = crossed(piece, axis_x)

    wide_y = own_y + 2 * halo
    span = 3 * own_x + edge
    q1, qy = (span - 4) // 2, (wide_y - 4) // 2
    h1_shape = jax.ShapeDtypeStruct((3, q1, 2, qy, depth, width), bf16)
    h2_shape = jax.ShapeDtypeStruct((3, q1, 2, qy - 1, depth, width), bf16)
    h3_shape = jax.ShapeDtypeStruct((q1 - 1, 2, qy - 2, depth, width), bf16)
    turned_shape = jax.ShapeDtypeStruct((span - 2, qy, depth, 128), bf16)
    tile = 2 * depth * 256 * 256

    size_y = blocks_in(own_y, count_y)
    box = (own_x, wide_y, (wide_y - size_y * own_y) // 2, size_y * own_y)
    energy = pl.pallas_call(
        functools.partial(energy_kernel, box),
        out_shape=jax.ShapeDtypeStruct((1, 1, 1, depth), f32),
        in_specs=[whole()] * 2,
        out_specs=whole(),
        compiler_params=granted(4),
        name="energy",
    )(strip, twin)

    rounds = box_rounds(2, size_y)
    plain = (count_x & (count_x - 1)) == 0 and (count_y & (count_y - 1)) == 0
    if plain:
        early = max(len(rounds) - 2, 0)
        for axis, step in rounds[:early]:
            energy = energy + shifted(energy, axis, step)
        e2, energy = lax.optimization_barrier((e2, energy))
        for axis, step in rounds[early : early + 1]:
            energy = energy + shifted(energy, axis, step)
    else:
        energy = lax.psum(energy, axis_x + (axis_y,)) / (2 * size_y)

    h1, turned, sides = pl.pallas_call(
        functools.partial(inner_kernel, edge),
        out_shape=(h1_shape, turned_shape, jax.ShapeDtypeStruct((2,) + strip.shape, f32)),
        in_specs=[scalar()] + [whole()] * 5,
        out_specs=(whole(),) * 3,
        scratch_shapes=[pltpu.VMEM((3 * own_x, 4 * wide_y, depth), f32)],
        cost_estimate=priced(4 * tile * q1 * qy),
        compiler_params=granted(12),
        name="inner",
    )(odd, apart, strip, twin, e1, bias1)

    turned, h1 = pl.pallas_call(
        functools.partial(outer_kernel, edge),
        out_shape=(turned_shape, h1_shape),
        in_specs=[scalar()] + [whole()] * 6,
        out_specs=(whole(), whole()),
        scratch_shapes=[pltpu.VMEM((edge + 2, 4 * wide_y, depth), f32)],
        input_output_aliases={5: 0, 6: 1},
        cost_estimate=priced(2 * tile * q1 * qy),
        compiler_params=granted(12),
        name="outer",
    )(odd, piece, sides, e1, bias1, turned, h1)

    h2, gift = pl.pallas_call(
        second_kernel,
        out_shape=(h2_shape, jax.ShapeDtypeStruct(h2_shape.shape[:1] + h2_shape.shape[2:], bf16)),
        in_specs=[scalar()] + [whole()] * 3,
        out_specs=(whole(), whole()),
        cost_estimate=priced(12 * tile * (q1 - 1) * (qy - 1)),
        compiler_params=granted(20),
        name="second",
    )(odd, h1, e2, bias2)
    gift, energy = lax.optimization_barrier((gift, energy))
    if plain:
        for axis, step in rounds[early + 1 :]:
            energy = energy + shifted(energy, axis, step)
    gift = swapped(gift, axis_x, 0)

    h3 = pl.pallas_call(
        alone_kernel,
        out_shape=h3_shape,
        in_specs=[scalar()] + [whole()] * 3,
        out_specs=whole(),
        cost_estimate=priced(12 * tile * (q1 - 2) * (qy - 2)),
        compiler_params=granted(20),
        name="third",
    )(odd, h2, e3, bias3)

    h2, h3 = pl.pallas_call(
        shared_kernel,
        out_shape=(h2_shape, h3_shape),
        in_specs=[scalar()] + [whole()] * 5,
        out_specs=(whole(), whole()),
        input_output_aliases={4: 0, 5: 1},
        cost_estimate=priced(12 * tile * (qy - 2)),
        compiler_params=granted(12),
        name="shared",
    )(odd, gift, e3, bias3, h2, h3)

    cells = own_x * own_y * depth * count_x * count_y

    return pl.pallas_call(
        functools.partial(final_kernel, cells),
        out_shape=(
            jax.ShapeDtypeStruct(v.shape, f32),
            jax.ShapeDtypeStruct((6,) + v.shape[1:], f32),
        ),
        in_specs=[whole()] * 5,
        out_specs=(whole(), whole()),
        scratch_shapes=[pltpu.VMEM((2 * (q1 - 2), 8 * 2 * (qy - 3), depth), f32)],
        cost_estimate=priced(8 * tile * (q1 - 2) * (qy - 3)),
        compiler_params=granted(10),
        name="final",
    )(h3, e4, strip, sides, energy)


def solution(mesh):
    block = P(None, axis_x, axis_y, None)
    return jax.shard_map(
        local,
        mesh=mesh,
        in_specs=(block,) + (P(),) * 7,
        out_specs=(block, block),
        check_vma=False,
    )
```

```python
import functools

import jax
import jax.numpy as jnp
from jax import lax
from jax.experimental import pallas as pl
from jax.experimental.pallas import tpu as pltpu
from jax.sharding import PartitionSpec as P

time_step = 0.1
viscosity = 0.05
power_input = 5.0
pairing = ((0, 3, 4), (3, 1, 5), (4, 5, 2))
halo = 6
axis_x = ("grp", "gx")
axis_y = "gy"
groups = 8
f32 = jnp.float32
bf16 = jnp.bfloat16


def shifted(cells, axis, step):
    count = lax.axis_size(axis)
    return lax.ppermute(cells, axis, [(i, (i + step) % count) for i in range(count)])


def swapped(cells, axis, odd):
    count = lax.axis_size(axis)
    order = [(i, (i + 1 if i % 2 == odd else i - 1) % count) for i in range(count)]
    return lax.ppermute(cells, axis, order)


def crossed(cells, axis):
    count = lax.axis_size(axis)
    return lax.ppermute(cells, axis, [(i, (i - 2 if i % 2 else i + 2) % count) for i in range(count)])


def blocks_in(extent, count):
    size = 1
    while count % (2 * size) == 0 and 2 * size * extent <= extent + 2 * halo:
        size *= 2
    return size


def expand_hidden(w_ref, out_ref):
    outs, channels = w_ref.shape[3], w_ref.shape[4]
    zero = jnp.zeros((outs, channels), f32)
    blank = jnp.zeros((channels, 2 * outs), bf16)
    for dz in range(3):
        for xin in range(4):
            tall = []
            for dy in range(3):
                rows = [
                    w_ref[xin - xo, dy, dz].astype(f32) if 0 <= xin - xo <= 2 else zero
                    for xo in range(2)
                ]
                tall.append(jnp.concatenate(rows, axis=0).T.astype(bf16))
            for yin in range(4):
                base = ((dz * 4 + yin) * 4 + xin) * channels
                for yo in range(2):
                    piece = tall[yin - yo] if 0 <= yin - yo <= 2 else blank
                    out_ref[base : base + channels, yo * 2 * outs : (yo + 1) * 2 * outs] = piece


def selector(yo):
    row = lax.broadcasted_iota(jnp.int32, (128, 128), 0)
    column = lax.broadcasted_iota(jnp.int32, (128, 128), 1)
    group, yin, part = row >> 4, (row >> 2) & 3, row & 3
    one, two = jnp.where(group >= 3, 1, 0), jnp.where(group >= 6, 1, 0)
    along = one + two
    dz = group - 3 * along
    spare = part == 3
    along = jnp.where(spare, 2, along)
    dz = jnp.where(spare, 2, dz)
    part = jnp.where(spare, group, part)
    wanted = (yin - yo) * 32 + (3 * part + along) * 3 + dz
    fits = (yin >= yo) & (yin - yo <= 2) & (part <= 2) & (column == wanted)
    return jnp.where(fits, 1.0, 0.0).astype(bf16)


def expand_first(w_ref, out_ref, flat):
    features, outs = w_ref.shape[2], w_ref.shape[4]
    flat[...] = jnp.zeros_like(flat)
    for dx in range(3):
        for dy in range(3):
            for channel in range(features):
                row = dy * 32 + channel * 3
                flat[dx, row : row + 3, :] = w_ref[dx, dy, channel].astype(f32)
    zero = jnp.zeros(flat.shape[1:], f32)
    for yo in range(2):
        pick = selector(yo)
        for xin in range(4):
            sides = [flat[xin - xo] if 0 <= xin - xo <= 2 else zero for xo in range(2)]
            both = jnp.concatenate(sides, axis=1).astype(bf16)
            block = jnp.dot(pick, both, preferred_element_type=f32)
            out_ref[xin * 128 : (xin + 1) * 128, yo * 2 * outs : (yo + 1) * 2 * outs] = (
                block.astype(bf16)
            )


def expand_last(w_ref, out_ref):
    outs, channels = w_ref.shape[3], w_ref.shape[4]
    zero = jnp.zeros((8, channels), f32)
    pad = jnp.zeros((8 - outs, channels), f32)
    for pair in range(2):
        column = []
        for dy in range(3):
            for dz in range(3):
                for xo in range(2):
                    halves = []
                    for dx in (2 * pair - xo, 2 * pair + 1 - xo):
                        if 0 <= dx <= 2:
                            tap = w_ref[dx, dy, dz].astype(f32)
                            halves.append(jnp.concatenate([tap, pad], axis=0))
                        else:
                            halves.append(zero)
                    column.append(jnp.concatenate(halves, axis=1))
        base = pair * 2 * channels
        out_ref[:, base : base + 2 * channels] = jnp.concatenate(column, axis=0).astype(bf16)


def first_kernel(w1, b1, out_ref, bias, flat):
    bias[...] = jnp.concatenate([b1[...]] * 4, axis=1)
    expand_first(w1, out_ref, flat)


def later_kernel(w2, w3, w4, o2, o3, o4):
    expand_hidden(w2, o2)
    expand_hidden(w3, o3)
    expand_last(w4, o4)


def ends_kernel(width, v, head, tail):
    parts, extent_x, extent_y = v.shape[:3]
    for c in range(parts):
        for x in range(extent_x):
            at = (c * extent_x + x) * width
            head[at : at + width, :] = v[c, x, 0:width, :]
            tail[at : at + width, :] = v[c, x, extent_y - width : extent_y, :]


def strip_kernel(odd, v, left, right, strip, piece):
    parts, extent_x, extent_y = v.shape[:3]
    width = left.shape[0] // (parts * extent_x)
    tall = extent_y + 2 * width
    for c in range(parts):
        for x in range(extent_x):
            source, at = (c * extent_x + x) * width, (c * extent_x + x) * tall
            middle = at + width
            strip[at:middle, :] = left[source : source + width, :]
            strip[middle : middle + extent_y, :] = v[c, x]
            strip[middle + extent_y : at + tall, :] = right[source : source + width, :]
    reach = piece.shape[0] // (parts * tall)
    size = reach * tall
    for c in range(parts):
        head = c * extent_x * tall
        tail = head + (extent_x - reach) * tall
        piece[c * size : (c + 1) * size, :] = jnp.where(
            odd[0] == 1, strip[head : head + size, :], strip[tail : tail + size, :]
        )


def energy_kernel(box, own, twin, energy):
    wide, tall, low, span = box
    total = None
    for piece in (own, twin):
        for k in range(3 * wide):
            part = piece[k * tall + low : k * tall + low + span, :]
            total = part * part if total is None else total + part * part
    energy[...] = jnp.broadcast_to(0.5 * jnp.sum(total, keepdims=True), energy.shape)


def whole():
    return pl.BlockSpec(memory_space=pltpu.VMEM)


def granted(mib):
    return pltpu.CompilerParams(vmem_limit_bytes=mib * 2**20)


def priced(flops):
    return pl.CostEstimate(flops=int(flops), bytes_accessed=10**6, transcendentals=0)


def ends(v, width):
    shape = jax.ShapeDtypeStruct((v.shape[0] * v.shape[1] * width, v.shape[3]), f32)
    return pl.pallas_call(
        functools.partial(ends_kernel, width),
        out_shape=(shape, shape),
        in_specs=[whole()],
        out_specs=(whole(), whole()),
        compiler_params=granted(4),
        name="ends",
    )(v)


def scalar():
    return pl.BlockSpec(memory_space=pltpu.SMEM)


def strips(odd, v, left, right, reach):
    parts, extent_x, extent_y, depth = v.shape
    tall = extent_y + 2 * halo
    return pl.pallas_call(
        strip_kernel,
        out_shape=(
            jax.ShapeDtypeStruct((parts * extent_x * tall, depth), f32),
            jax.ShapeDtypeStruct((parts * reach * tall, depth), f32),
        ),
        in_specs=[scalar()] + [whole()] * 3,
        out_specs=(whole(), whole()),
        compiler_params=granted(4),
        name="strips",
    )(odd, v, left, right)


def prepare_first(w1, b1):
    outs = w1.shape[3]
    w1 = jnp.transpose(w1, (0, 1, 4, 2, 3))
    return pl.pallas_call(
        first_kernel,
        out_shape=(
            jax.ShapeDtypeStruct((512, 4 * outs), bf16),
            jax.ShapeDtypeStruct((1, 4 * outs), f32),
        ),
        in_specs=[whole()] * 2,
        out_specs=(whole(),) * 2,
        scratch_shapes=[pltpu.VMEM((3, 128, outs), f32)],
        cost_estimate=pl.CostEstimate(flops=4 * 10**9, bytes_accessed=10**7, transcendentals=0),
        compiler_params=granted(10),
        name="prepare_first",
    )(w1, b1.reshape(1, -1))


def prepare_later(w2, w3, w4):
    outs, channels = w2.shape[3], w2.shape[4]
    return pl.pallas_call(
        later_kernel,
        out_shape=(
            jax.ShapeDtypeStruct((48 * channels, 4 * outs), bf16),
            jax.ShapeDtypeStruct((48 * channels, 4 * outs), bf16),
            jax.ShapeDtypeStruct((144, 4 * channels), bf16),
        ),
        in_specs=[whole()] * 3,
        out_specs=(whole(),) * 3,
        cost_estimate=priced(10**9),
        compiler_params=granted(10),
        name="prepare_later",
    )(w2, w3, w4)


def lay_rows(target, at, piece, x, wide, tall):
    for c in range(3):
        start = (c * wide + x) * tall
        target[at, pl.ds(c, tall, stride=4), :] = piece[start : start + tall, :]
    target[at, pl.ds(3, tall, stride=4), :] = jnp.zeros((tall, piece.shape[1]), f32)


def features(rows, at, depth):
    total = rows.shape[1]
    center = rows[at + 1, 4 : total - 4, :]
    diffs = (
        (rows[at + 2, 4 : total - 4, :] - rows[at, 4 : total - 4, :]) * 0.5,
        (rows[at + 1, 8:total, :] - rows[at + 1, 0 : total - 8, :]) * 0.5,
        (pltpu.roll(center, depth - 1, 1) - pltpu.roll(center, 1, 1)) * 0.5,
    )
    parts = []
    for j in range(3):
        for amount in (1, 0, depth - 1):
            parts.append(pltpu.roll(diffs[j], amount, 1) if amount else diffs[j])
    spare = parts.pop()
    lane = lax.broadcasted_iota(jnp.int32, spare.shape, 0) & 3
    for c in range(3):
        parts[c] = jnp.where(lane == 3, pltpu.roll(spare, 3 - c, 0), parts[c])
    turned = []
    for half in range((total // 4 - 2) // 2 - 1):
        block = jnp.concatenate([part[8 * half : 8 * half + 16] for part in parts], axis=0)
        turned.append(block.astype(bf16).T)
    return turned


def merge(block):
    return block.reshape((block.shape[0] * block.shape[1],) + block.shape[2:])


def layer(left, weight, bias, store, depth, variants):
    total = jnp.dot(left, weight[...], preferred_element_type=f32)
    value = jnp.tanh(total + bias)
    value = value.reshape(value.shape[0] // depth, depth, value.shape[1])
    width = value.shape[2] // 2
    for dz, amount in enumerate((1, 0, depth - 1)):
        if dz not in variants:
            continue
        moved = pltpu.roll(value, amount, 1) if amount else value
        moved = moved.astype(bf16)
        for yo in range(2):
            store(dz, yo, moved[:, :, yo * width : (yo + 1) * width])


every = (0, 1, 2)


def gather_hidden(source, xp, variants):
    rows = source.shape[-3] - 1
    parts = []
    for dz in variants:
        for yin in range(4):
            for pair in range(2):
                where = (xp + pair, yin % 2, slice(yin // 2, yin // 2 + rows))
                parts.append(merge(source[where if len(source.shape) == 5 else (dz, *where)]))
    return jnp.concatenate(parts, axis=1)


def store_hidden(target, xp):
    def store(dz, yo, block):
        target[(xp, yo) if len(target.shape) == 5 else (dz, xp, yo)] = block

    return store


def inner_kernel(edge, odd, apart, own, twin, w1, bias, h1, turned, sides, rows):
    depth, tall = own.shape[1], rows.shape[1] // 4
    wide = own.shape[0] // (3 * tall)
    right = odd[0]
    sides[right] = apart[...]
    sides[1 - right] = twin[...]
    for piece, at in ((apart, right * 2 * wide), (own, wide), (twin, (1 - right) * 2 * wide)):
        for x in range(wide):
            lay_rows(rows, at + x, piece, x, wide, tall)
    first = (1 - right) * edge
    inside = turned.shape[0] - edge

    def one(x, carry):
        for half, block in enumerate(features(rows, x, depth)):
            turned[x + first, half] = block
        return carry

    lax.fori_loop(0, inside, one, 0, unroll=True)
    low = (1 - right) * (edge // 2)

    def step(q, carry):
        left = jnp.concatenate([merge(turned[2 * q + first + a]) for a in range(4)], axis=1)
        layer(left, w1, bias[...], store_hidden(h1, q + low), depth, every)
        return carry

    lax.fori_loop(0, inside // 2 - 1, step, 0, unroll=True)


def outer_kernel(edge, odd, piece, sides, w1, bias, _, __, turned, h1, rows):
    depth, tall = piece.shape[1], rows.shape[1] // 4
    reach = piece.shape[0] // (3 * tall)
    wide = sides.shape[1] // (3 * tall)
    right = odd[0]
    for x in range(reach):
        lay_rows(rows, right * 2 + x, piece, x, reach, tall)
    near = sides.at[right]
    for x in range(2):
        for c in range(3):
            head = (c * wide + x) * tall
            tail = (c * wide + wide - 2 + x) * tall
            value = jnp.where(right == 1, near[tail : tail + tall, :], near[head : head + tall, :])
            rows[(1 - right) * reach + x, pl.ds(c, tall, stride=4), :] = value
        rows[(1 - right) * reach + x, pl.ds(3, tall, stride=4), :] = jnp.zeros((tall, depth), f32)
    base = right * (turned.shape[0] - edge)
    for at in range(edge):
        for half, block in enumerate(features(rows, at, depth)):
            turned[base + at, half] = block
    start = right * (turned.shape[0] - 2 - edge)
    for k in range(edge // 2):
        left = jnp.concatenate([merge(turned[start + 2 * k + a]) for a in range(4)], axis=1)
        xp = right * (h1.shape[1] - edge // 2) + k
        layer(left, w1, bias[...], store_hidden(h1, xp), depth, every)


def second_kernel(odd, h1, w2, bias, h2, gift):
    depth = h1.shape[4]

    def step(xp, carry):
        store = store_hidden(h2, xp + odd[0])
        layer(gather_hidden(h1, xp, every), w2, jnp.concatenate([bias[...]] * 4, axis=1), store, depth, every)
        return carry

    lax.fori_loop(0, h2.shape[1] - 1, step, 0, unroll=True)
    gift[...] = h2[:, h2.shape[1] // 2]


def alone_kernel(odd, h2, w3, bias, h3):
    depth = h2.shape[4]

    def step(k, carry):
        xp = k + odd[0]
        store = store_hidden(h3, xp)
        layer(gather_hidden(h2, xp, every), w3, jnp.concatenate([bias[...]] * 4, axis=1), store, depth, (1,))
        return carry

    lax.fori_loop(0, h3.shape[0] - 1, step, 0, unroll=True)


def shared_kernel(odd, gift, w3, bias, _, __, h2, h3):
    depth = h2.shape[4]
    h2[:, (1 - odd[0]) * (h2.shape[1] - 1)] = gift[...]
    xp = (1 - odd[0]) * (h3.shape[0] - 1)
    store = store_hidden(h3, xp)
    layer(gather_hidden(h2, xp, every), w3, jnp.concatenate([bias[...]] * 4, axis=1), store, depth, (1,))


def final_kernel(cells, h3, w4, own, sides, energy, updated_ref, stress_ref, tau):
    near, far = sides.at[0], sides.at[1]
    depth = own.shape[1]
    forcing = power_input / (2.0 * (energy[0, 0] / cells) + 1e-06)

    rows = h3.shape[2]

    def final(xp, carry):
        cells = [merge(merge(h3[xp + pair])) for pair in range(2)]
        sides = lax.dot_general(
            w4[...],
            jnp.concatenate(cells, axis=1),
            (((1,), (1,)), ((), ())),
            preferred_element_type=f32,
        )
        for y in range(2 * rows - 2):
            sums = []
            for dz in range(3):
                total = None
                for dy in range(3):
                    at = ((y + dy) % 2 * rows + (y + dy) // 2) * depth
                    tap = (3 * dy + dz) * 16
                    part = sides[tap : tap + 16, at : at + depth]
                    total = part if total is None else total + part
                sums.append(total)
            total = pltpu.roll(sums[0], 1, 1) + sums[1] + pltpu.roll(sums[2], depth - 1, 1)
            for xo in range(2):
                tau[2 * xp + xo, y * 8 : y * 8 + 8, :] = total[xo * 8 : xo * 8 + 8]
        return carry

    lax.fori_loop(0, h3.shape[0] - 1, final, 0, unroll=True)

    own_x, own_y = updated_ref.shape[1], updated_ref.shape[2]

    def stress_at(c, x, y):
        return tau[x, pl.ds(y * 8 + c, own_y, stride=8), :]

    def turn(a, amount):
        return pltpu.roll(a, amount % depth, 1)

    def vel(i, x, y):
        piece, at = own, x
        if x < 0:
            piece, at = near, x + own_x
        elif x >= own_x:
            piece, at = far, x - own_x
        start = (i * own_x + at) * (own_y + 2 * halo) + halo + y
        return piece[start : start + own_y, :]

    for x in range(own_x):
        for c in range(6):
            stress_ref[c, x] = stress_at(c, x + 1, 1)
        center = [vel(i, x, 0) for i in range(3)]
        for i in range(3):
            xm, xp, ym, yp = vel(i, x - 1, 0), vel(i, x + 1, 0), vel(i, x, -1), vel(i, x, 1)
            zm, zp = turn(center[i], 1), turn(center[i], -1)
            advect = (
                center[0] * ((xp - xm) * 0.5)
                + center[1] * ((yp - ym) * 0.5)
                + center[2] * ((zp - zm) * 0.5)
            )
            laplacian = xp + xm + yp + ym + zm + zp - 6.0 * center[i]
            px, py, pz = pairing[i]
            along_z = stress_at(pz, x + 1, 1)
            divergence = (
                (stress_at(px, x + 2, 1) - stress_at(px, x, 1)) * 0.5
                + (stress_at(py, x + 1, 2) - stress_at(py, x + 1, 0)) * 0.5
                + (turn(along_z, -1) - turn(along_z, 1)) * 0.5
            )
            tendency = viscosity * laplacian - advect - divergence + forcing * center[i]
            updated_ref[i, x] = center[i] + time_step * tendency


def box_rounds(size_x, size_y):
    count_x, count_y = lax.axis_size(axis_x), lax.axis_size(axis_y)
    rounds = []
    while size_y < count_y:
        rounds.append((axis_y, size_y))
        size_y *= 2
    while size_x < count_x:
        rounds.append((axis_x, size_x))
        size_x *= 2
    return rounds


def local(v, w1, b1, w2, b2, w3, b3, w4):
    parts, own_x, own_y, depth = v.shape
    count_x, count_y = lax.axis_size(axis_x), lax.axis_size(axis_y)
    width = 2 * w2.shape[3]
    bias2, bias3 = b2.reshape(1, -1), b3.reshape(1, -1)
    odd = (lax.axis_index(axis_x) % 2).reshape(1)
    head, tail = ends(v, halo)
    left, right = shifted(tail, axis_y, 1), shifted(head, axis_y, -1)
    e1, bias1 = prepare_first(w1, b1)
    left, right, e1, bias1 = lax.optimization_barrier((left, right, e1, bias1))
    edge = halo - own_x
    strip, piece = strips(odd, v, left, right, edge)
    w2, w3, w4, strip = lax.optimization_barrier((w2, w3, w4, strip))
    e2, e3, e4 = prepare_later(w2, w3, w4)
    apart, twin = swapped(strip, axis_x, 1), swapped(strip, axis_x, 0)
    piece = crossed(piece, axis_x)

    wide_y = own_y + 2 * halo
    span = 3 * own_x + edge
    q1, qy = (span - 4) // 2, (wide_y - 4) // 2
    h1_shape = jax.ShapeDtypeStruct((3, q1, 2, qy, depth, width), bf16)
    h2_shape = jax.ShapeDtypeStruct((3, q1, 2, qy - 1, depth, width), bf16)
    h3_shape = jax.ShapeDtypeStruct((q1 - 1, 2, qy - 2, depth, width), bf16)
    turned_shape = jax.ShapeDtypeStruct((span - 2, qy, depth, 128), bf16)
    tile = 2 * depth * 256 * 256

    size_y = blocks_in(own_y, count_y)
    box = (own_x, wide_y, (wide_y - size_y * own_y) // 2, size_y * own_y)
    energy = pl.pallas_call(
        functools.partial(energy_kernel, box),
        out_shape=jax.ShapeDtypeStruct((1, 1, 1, depth), f32),
        in_specs=[whole()] * 2,
        out_specs=whole(),
        compiler_params=granted(4),
        name="energy",
    )(strip, twin)

    rounds = box_rounds(2, size_y)
    plain = (count_x & (count_x - 1)) == 0 and (count_y & (count_y - 1)) == 0
    if plain:
        early = max(len(rounds) - 2, 0)
        for axis, step in rounds[:early]:
            energy = energy + shifted(energy, axis, step)
        e2, energy = lax.optimization_barrier((e2, energy))
        for axis, step in rounds[early : early + 1]:
            energy = energy + shifted(energy, axis, step)
    else:
        energy = lax.psum(energy, axis_x + (axis_y,)) / (2 * size_y)

    h1, turned, sides = pl.pallas_call(
        functools.partial(inner_kernel, edge),
        out_shape=(h1_shape, turned_shape, jax.ShapeDtypeStruct((2,) + strip.shape, f32)),
        in_specs=[scalar()] + [whole()] * 5,
        out_specs=(whole(),) * 3,
        scratch_shapes=[pltpu.VMEM((3 * own_x, 4 * wide_y, depth), f32)],
        cost_estimate=priced(4 * tile * q1 * qy),
        compiler_params=granted(12),
        name="inner",
    )(odd, apart, strip, twin, e1, bias1)

    turned, h1 = pl.pallas_call(
        functools.partial(outer_kernel, edge),
        out_shape=(turned_shape, h1_shape),
        in_specs=[scalar()] + [whole()] * 6,
        out_specs=(whole(), whole()),
        scratch_shapes=[pltpu.VMEM((edge + 2, 4 * wide_y, depth), f32)],
        input_output_aliases={5: 0, 6: 1},
        cost_estimate=priced(2 * tile * q1 * qy),
        compiler_params=granted(12),
        name="outer",
    )(odd, piece, sides, e1, bias1, turned, h1)

    h2, gift = pl.pallas_call(
        second_kernel,
        out_shape=(h2_shape, jax.ShapeDtypeStruct(h2_shape.shape[:1] + h2_shape.shape[2:], bf16)),
        in_specs=[scalar()] + [whole()] * 3,
        out_specs=(whole(), whole()),
        cost_estimate=priced(12 * tile * (q1 - 1) * (qy - 1)),
        compiler_params=granted(20),
        name="second",
    )(odd, h1, e2, bias2)
    gift, energy = lax.optimization_barrier((gift, energy))
    if plain:
        for axis, step in rounds[early + 1 :]:
            energy = energy + shifted(energy, axis, step)
    gift = swapped(gift, axis_x, 0)

    h3 = pl.pallas_call(
        alone_kernel,
        out_shape=h3_shape,
        in_specs=[scalar()] + [whole()] * 3,
        out_specs=whole(),
        cost_estimate=priced(12 * tile * (q1 - 2) * (qy - 2)),
        compiler_params=granted(20),
        name="third",
    )(odd, h2, e3, bias3)

    h2, h3 = pl.pallas_call(
        shared_kernel,
        out_shape=(h2_shape, h3_shape),
        in_specs=[scalar()] + [whole()] * 5,
        out_specs=(whole(), whole()),
        input_output_aliases={4: 0, 5: 1},
        cost_estimate=priced(12 * tile * (qy - 2)),
        compiler_params=granted(12),
        name="shared",
    )(odd, gift, e3, bias3, h2, h3)

    cells = own_x * own_y * depth * count_x * count_y

    return pl.pallas_call(
        functools.partial(final_kernel, cells),
        out_shape=(
            jax.ShapeDtypeStruct(v.shape, f32),
            jax.ShapeDtypeStruct((6,) + v.shape[1:], f32),
        ),
        in_specs=[whole()] * 5,
        out_specs=(whole(), whole()),
        scratch_shapes=[pltpu.VMEM((2 * (q1 - 2), 8 * 2 * (qy - 3), depth), f32)],
        cost_estimate=priced(8 * tile * (q1 - 2) * (qy - 3)),
        compiler_params=granted(10),
        name="final",
    )(h3, e4, strip, sides, energy)


def solution(mesh):
    block = P(None, axis_x, axis_y, None)
    return jax.shard_map(
        local,
        mesh=mesh,
        in_specs=(block,) + (P(),) * 7,
        out_specs=(block, block),
        check_vma=False,
    )
```
